32 devices in a mesh: data: 4 (over z), stage: 8 (over y, x, core).
Axes of the slice: x: 2, y: 2, z: 4, core: 2. Of those that a mesh axis runs over, the one named last changes fastest.
Arguments:
- w_in: float32 [8, 768, 3072], P('stage')
- w_out: float32 [8, 3072, 768], P('stage')
- mom_in: float32 [8, 768, 3072], P('stage')
- mom_out: float32 [8, 3072, 768], P('stage')
- sq_in: float32 [8, 768, 3072], P('stage')
- sq_out: float32 [8, 3072, 768], P('stage')
- acc_in: float32 [4, 8, 768, 3072], P('data', 'stage')
- acc_out: float32 [4, 8, 3072, 768], P('data', 'stage')
- stage_acts: bfloat16 [8, 256, 768], P('stage', 'data')
- grad_y: bfloat16 [256, 768], P('data')
- x_next: bfloat16 [1, 256, 768], P(None, 'data')
- max_norm: float32 [], replicated
Outputs:
- output 1: float32 [8, 768, 3072], P('stage')
- output 2: float32 [8, 3072, 768], P('stage')
- output 3: float32 [8, 768, 3072], P('stage')
- output 4: float32 [8, 3072, 768], P('stage')
- output 5: float32 [8, 768, 3072], P('stage')
- output 6: float32 [8, 3072, 768], P('stage')
- output 7: bfloat16 [1, 256, 768], P(None, 'data')
All inputs are finite; a program needn't handle non-finite values.
Results may differ from the reference program's by a relative error of at most 0.0138451.
Values are sent between devices in bfloat16 or wider.
A program may use at most 1 GiB of HBM per device.

```python
import jax
import jax.numpy as jnp
from jax import lax

D = 768
FF = 3072
STAGES = 8
REPLICAS = 4
TOKENS = 64
NEXT_MB = 1
STEP_COUNT = 20

BETA_ONE = 0.9
BETA_TWO = 0.95
ADAM_EPS = 1e-8
WEIGHT_DECAY = 0.1
LR_GAIN = 0.2
CLIP_EPS = 1e-6
OUT_GAIN = 1.5


def gelu_back(pre_act, grad_h):
    return jax.vjp(jax.nn.gelu, pre_act)[1](grad_h)[0]


def stage_forward(x_in, w_first, w_second):
    pre_act = jnp.dot(x_in, w_first, preferred_element_type=jnp.float32)
    hidden = jax.nn.gelu(pre_act).astype(jnp.bfloat16)
    return jnp.dot(hidden, w_second, preferred_element_type=jnp.float32).astype(jnp.bfloat16)


def last_backward(w_in, w_out, stage_acts, grad_y):
    def body(grad_cur, layer):
        w_first, w_second, x_in = layer
        pre_act = jnp.dot(x_in, w_first, preferred_element_type=jnp.float32)
        hidden = jax.nn.gelu(pre_act).astype(jnp.bfloat16)
        grad_h = jnp.dot(grad_cur, w_second.T, preferred_element_type=jnp.float32)
        grad_pre = gelu_back(pre_act, grad_h).astype(jnp.bfloat16)
        grad_second = jnp.dot(hidden.T, grad_cur, preferred_element_type=jnp.float32)
        grad_first = jnp.dot(x_in.T, grad_pre, preferred_element_type=jnp.float32)
        grad_next = jnp.dot(grad_pre, w_first.T, preferred_element_type=jnp.float32).astype(jnp.bfloat16)
        return grad_next, (grad_first, grad_second)

    layers = (w_in.astype(jnp.bfloat16), w_out.astype(jnp.bfloat16), stage_acts)
    _, grads = lax.scan(body, grad_y, layers, reverse=True)
    return grads


def adamw_update(weight, moment, sq_moment, gradient, learn_rate):
    moment_new = BETA_ONE * moment + (1.0 - BETA_ONE) * gradient
    sq_new = BETA_TWO * sq_moment + (1.0 - BETA_TWO) * gradient * gradient
    m_hat = moment_new / (1.0 - BETA_ONE ** STEP_COUNT)
    v_hat = sq_new / (1.0 - BETA_TWO ** STEP_COUNT)
    weight_new = weight * (1.0 - learn_rate * WEIGHT_DECAY) - learn_rate * m_hat / (jnp.sqrt(v_hat) + ADAM_EPS)
    return weight_new, moment_new, sq_new


def setup_inputs(seed: int = 0) -> dict:
    keys = jax.random.split(jax.random.key(seed), 12)
    rows = REPLICAS * TOKENS
    w_in = jax.random.normal(keys[0], (STAGES, D, FF), jnp.float32) * D ** -0.5
    w_out = jax.random.normal(keys[1], (STAGES, FF, D), jnp.float32) * (OUT_GAIN * FF ** -0.5)
    stage_acts = jax.random.normal(keys[2], (STAGES, rows, D), jnp.float32).astype(jnp.bfloat16)
    grad_y = (jax.random.normal(keys[3], (rows, D), jnp.float32) * rows ** -0.5).astype(jnp.bfloat16)
    x_next = jax.random.normal(keys[4], (NEXT_MB, rows, D), jnp.float32).astype(jnp.bfloat16)
    grad_first, grad_second = last_backward(w_in, w_out, stage_acts, grad_y)
    scale_in = jnp.sqrt(jnp.mean(grad_first * grad_first) / REPLICAS)
    scale_out = jnp.sqrt(jnp.mean(grad_second * grad_second) / REPLICAS)
    acc_in = jax.random.normal(keys[5], (REPLICAS, STAGES, D, FF), jnp.float32) * scale_in
    acc_out = jax.random.normal(keys[6], (REPLICAS, STAGES, FF, D), jnp.float32) * scale_out
    avg_in = (jnp.sum(acc_in, axis=0) + grad_first) / REPLICAS
    avg_out = (jnp.sum(acc_out, axis=0) + grad_second) / REPLICAS
    full_norm = jnp.sqrt(jnp.sum(avg_in * avg_in) + jnp.sum(avg_out * avg_out))
    ratio = jax.random.uniform(keys[7], (), jnp.float32, 0.35, 0.65)
    max_norm = ratio * full_norm
    level_in = ratio * jnp.sqrt(jnp.mean(avg_in * avg_in, axis=(1, 2), keepdims=True))
    level_out = ratio * jnp.sqrt(jnp.mean(avg_out * avg_out, axis=(1, 2), keepdims=True))
    mom_in = jax.random.normal(keys[8], (STAGES, D, FF), jnp.float32) * (0.12 * level_in)
    mom_out = jax.random.normal(keys[9], (STAGES, FF, D), jnp.float32) * (0.12 * level_out)
    sq_in = jax.random.uniform(keys[10], (STAGES, D, FF), jnp.float32, 0.5, 1.5) * (0.05 * level_in * level_in)
    sq_out = jax.random.uniform(keys[11], (STAGES, FF, D), jnp.float32, 0.5, 1.5) * (0.05 * level_out * level_out)
    return dict(w_in=w_in, w_out=w_out, mom_in=mom_in, mom_out=mom_out, sq_in=sq_in, sq_out=sq_out, acc_in=acc_in, acc_out=acc_out, stage_acts=stage_acts, grad_y=grad_y, x_next=x_next, max_norm=max_norm)


def reference(w_in, w_out, mom_in, mom_out, sq_in, sq_out, acc_in, acc_out, stage_acts, grad_y, x_next, max_norm):
    grad_first, grad_second = last_backward(w_in, w_out, stage_acts, grad_y)
    avg_in = (jnp.sum(acc_in, axis=0) + grad_first) / REPLICAS
    avg_out = (jnp.sum(acc_out, axis=0) + grad_second) / REPLICAS
    sq_norm = jnp.sum(avg_in * avg_in) + jnp.sum(avg_out * avg_out)
    clip_factor = jnp.minimum(1.0, max_norm / (jnp.sqrt(sq_norm) + CLIP_EPS))
    learn_rate = LR_GAIN * D ** -0.5
    new_in, mom_in_new, sq_in_new = adamw_update(w_in, mom_in, sq_in, clip_factor * avg_in, learn_rate)
    new_out, mom_out_new, sq_out_new = adamw_update(w_out, mom_out, sq_out, clip_factor * avg_out, learn_rate)
    layers = (new_in.astype(jnp.bfloat16), new_out.astype(jnp.bfloat16))

    def run_micro(x_mb):
        def body(x_cur, layer):
            return stage_forward(x_cur, layer[0], layer[1]), None
        y_last, _ = lax.scan(body, x_mb, layers)
        return y_last

    y_next = lax.map(run_micro, x_next)
    return new_in, new_out, mom_in_new, mom_out_new, sq_in_new, sq_out_new, y_next
```

```python
import math

import jax
import jax.numpy as jnp
from jax import lax
from jax.experimental import pallas as pl
from jax.experimental.pallas import tpu as pltpu
from jax.sharding import PartitionSpec as P

BETA_ONE = 0.9
BETA_TWO = 0.95
ADAM_EPS = 1e-8
WEIGHT_DECAY = 0.1
LR_GAIN = 0.2
CLIP_EPS = 1e-6
STEP_COUNT = 20
MESH = pl.DeviceIdType.MESH
F32, BF16 = jnp.float32, jnp.bfloat16

D, FF, STAGES, REPLICAS, TOK = 768, 3072, 8, 4, 64
ROWS = REPLICAS * TOK
CHUNKS = 24
R1, R2 = D // CHUNKS, FF // CHUNKS
TILE = 256
SLOTS = 8
EARLY = 4
LEARN_RATE = LR_GAIN * D ** -0.5
GELU_K = math.sqrt(2.0 / math.pi)
NT = (((1,), (1,)), ((), ()))
TN = (((0,), (0,)), ((), ()))
NN = (((1,), (0,)), ((), ()))


def mm(lhs, rhs, dims):
    return lax.dot_general(lhs, rhs, dims, preferred_element_type=F32)


def gelu_parts(z):
    zz = z * z
    tanh = jnp.tanh(GELU_K * (z + 0.044715 * (zz * z)))
    cdf = 0.5 * (1.0 + tanh)
    slope = cdf + (0.5 * z) * (1.0 - tanh * tanh) * (GELU_K * (1.0 + (3 * 0.044715) * zz))
    return z * cdf, slope


def gelu(z):
    return z * (0.5 * (1.0 + jnp.tanh(GELU_K * (z + 0.044715 * (z * z * z)))))


def clip_of(sq_norm, max_norm):
    return jnp.minimum(1.0, max_norm / (jnp.sqrt(sq_norm) + CLIP_EPS))


def adamw(weight, moment, sq_moment, gradient):
    moment_new = BETA_ONE * moment + (1.0 - BETA_ONE) * gradient
    sq_new = BETA_TWO * sq_moment + (1.0 - BETA_TWO) * gradient * gradient
    m_hat = moment_new / (1.0 - BETA_ONE ** STEP_COUNT)
    v_hat = sq_new / (1.0 - BETA_TWO ** STEP_COUNT)
    weight_new = weight * (1.0 - LEARN_RATE * WEIGHT_DECAY) - LEARN_RATE * m_hat / (jnp.sqrt(v_hat) + ADAM_EPS)
    return weight_new, moment_new, sq_new


def owner_of(stage):
    return 3 * ((stage % 2 + (stage // 2) % 2) % 2)


def ds(index, size):
    return pl.ds(pl.multiple_of(index * size, size), size)


def step_kernel(w1, w2, m1, m2, v1, v2, acc1, acc2, a_in, gy_in, x_in, maxn,
                g1_o, g2_o, nrm_o, y_o,
                recv1, recv2, own1, own2, b1, b2, gp, hid, dz, abuf, gbuf, gnext, xbuf, ybuf, sq1, sq2, nbuf, nres,
                a_snd, a_rcv, in_snd, in_rcv, g_snd, g_rcv, x_snd, x_rcv, y_snd, y_rcv, rs_snd, rs_rcv, ag_snd, ag_rcv,
                n_snd, n_rcv, nt_snd, nt_rcv, ld, st, loc):
    r = lax.axis_index("data")
    s = lax.axis_index("stage")
    own_r = owner_of(s)
    away = 1 - 2 * (own_r // 3)
    d = (r - own_r) * away
    accs, recvs, owns, gouts = (acc1, acc2), (recv1, recv2), (own1, own2), (g1_o, g2_o)
    heights = (R1, R2)

    def remote(src, dst, snd, rcv, to_r, to_s):
        return pltpu.make_async_remote_copy(src_ref=src, dst_ref=dst, send_sem=snd, recv_sem=rcv,
                                            device_id=(to_r, to_s), device_id_type=MESH)

    def arrive(ref, sem):
        pltpu.make_async_copy(ref, ref, sem).wait()

    def gather(src, dst, snd, rcv):
        part = dst.at[ds(r, TOK), :]

        @pl.when(d == 0)
        def _():
            pltpu.make_async_copy(src, part, rcv.at[r]).start()

        @pl.when(d != 0)
        def _():
            remote(src, part, snd, rcv.at[r], own_r, s).start()

    def gathered(dst, rcv):
        for q in range(REPLICAS):
            arrive(dst.at[pl.ds(q * TOK, TOK), :], rcv.at[q])

    @pl.when(s == STAGES - 1)
    def _():
        gather(gy_in, gbuf, in_snd, in_rcv)

    gather(a_in, abuf, a_snd, a_rcv)

    @pl.when(s == 0)
    def _():
        gather(x_in, xbuf, in_snd, in_rcv)

    def rs_copy(mat, k, src):
        part = recvs[mat].at[ds(k, heights[mat]), :]
        sem = mat * CHUNKS + k
        return remote(src, part, rs_snd.at[sem], rs_rcv.at[sem], r - away, s)

    def rs_src(mat, k):
        return accs[mat].at[0, 0, ds(k, heights[mat]), :]

    def ag_copy(mat, k, from_vmem):
        rows = ds(k, heights[mat])
        src = recvs[mat] if from_vmem else gouts[mat]
        sem = mat * CHUNKS + k
        return remote(src.at[rows, :], gouts[mat].at[rows, :], ag_snd.at[sem], ag_rcv.at[sem], r + away, s)

    def each(mats, fn, lo=0, hi=CHUNKS):
        for mat in mats:
            @pl.loop(lo, hi)
            def _(k):
                fn(mat, k)

    @pl.when(d == 3)
    def _():
        each((0, 1), lambda mat, k: rs_copy(mat, k, rs_src(mat, k)).start())

    @pl.when((d == 1) | (d == 2))
    def _():
        own_copies = [pltpu.make_async_copy(accs[mat].at[0, 0], owns[mat], ld.at[mat, 0]) for mat in (0, 1)]
        for copy in own_copies:
            copy.start()
        for mat in (0, 1):
            own_copies[mat].wait()

            @pl.loop(0, CHUNKS)
            def _(k):
                rows = ds(k, heights[mat])
                arrive(recvs[mat].at[rows, :], rs_rcv.at[mat * CHUNKS + k])
                recvs[mat][rows, :] = recvs[mat][rows, :] + owns[mat][rows, :]
                rs_copy(mat, k, recvs[mat].at[rows, :]).start()

    @pl.when(d != 0)
    def _():
        for mat in (0, 1):
            @pl.loop(0, CHUNKS)
            def _(k):
                rows = ds(k, heights[mat])
                arrive(gouts[mat].at[rows, :], ag_rcv.at[mat * CHUNKS + k])

                @pl.when(d != 3)
                def _():
                    ag_copy(mat, k, False).start()

                if mat == 1:
                    @pl.when((s == STAGES - 1) & (k == CHUNKS - 8))
                    def _():
                        arrive(y_o, y_rcv)
                        for t in range(1, STAGES):
                            remote(y_o, y_o, y_snd.at[t], y_rcv, r, (s + t) % STAGES).start()

        arrive(nres, nt_rcv)
        remote(a_in, abuf.at[ds(r, TOK), :], a_snd, a_rcv.at[r], own_r, s).wait_send()

        @pl.when((s == 0) | (s == STAGES - 1))
        def _():
            remote(x_in, xbuf.at[ds(r, TOK), :], in_snd, in_rcv.at[r], own_r, s).wait_send()

        each((0, 1), lambda mat, k: rs_copy(mat, k, rs_src(mat, k)).wait_send())

        @pl.when(d != 3)
        def _():
            each((0, 1), lambda mat, k: ag_copy(mat, k, False).wait_send())

    @pl.when(d == 0)
    def _():
        loads = [pltpu.make_async_copy(w.at[0], own, ld.at[mat, 0]) for mat, (w, own) in enumerate(((w1, own1), (w2, own2)))]
        for copy in loads:
            copy.start()
        sq1[...] = jnp.zeros_like(sq1)
        sq2[...] = jnp.zeros_like(sq2)
        loads[0].wait()

        @pl.loop(0, CHUNKS)
        def _(k):
            b1[ds(k, R1), :] = own1[ds(k, R1), :].astype(BF16)

        loads[1].wait()

        @pl.loop(0, CHUNKS)
        def _(k):
            b2[ds(k, R2), :] = own2[ds(k, R2), :].astype(BF16)

        own_copies = [pltpu.make_async_copy(accs[mat].at[0, 0], owns[mat], ld.at[mat, 1]) for mat in (0, 1)]
        for copy in own_copies:
            copy.start()

        gathered(abuf, a_rcv)

        @pl.loop(0, FF // TILE)
        def _(j):
            cols = ds(j, TILE)
            value, slope = gelu_parts(mm(abuf[...], b1[:, cols], NN))
            hid[:, cols] = value.astype(BF16)
            gp[:, cols] = slope

        @pl.when(s == STAGES - 1)
        def _():
            gathered(gbuf, in_rcv)

        @pl.when(s != STAGES - 1)
        def _():
            arrive(gbuf, g_rcv)

        @pl.loop(0, FF // TILE)
        def _(j):
            cols = ds(j, TILE)
            dz[:, cols] = (gp[:, cols] * mm(gbuf[...], b2[cols, :], NT)).astype(BF16)

        send_g = remote(gnext, gbuf, g_snd, g_rcv, owner_of(s + STAGES - 1), (s + STAGES - 1) % STAGES)

        @pl.when(s != 0)
        def _():
            @pl.loop(0, D // TILE)
            def _(j):
                gnext[:, ds(j, TILE)] = mm(dz[...], b1[ds(j, TILE), :], NT).astype(BF16)

            send_g.start()

        own_copies[0].wait()

        @pl.loop(0, FF // TILE)
        def _(j):
            cols = ds(j, TILE)
            own1[:, cols] = own1[:, cols] + mm(abuf[...], dz[:, cols], TN)

        own_copies[1].wait()

        @pl.loop(0, FF // TILE)
        def _(j):
            cols = ds(j, TILE)
            own2[cols, :] = own2[cols, :] + mm(hid[:, cols], gbuf[...], TN)

        for mat in (0, 1):
            sq = (sq1, sq2)[mat]

            @pl.loop(0, CHUNKS)
            def _(k):
                rows = ds(k, heights[mat])
                arrive(recvs[mat].at[rows, :], rs_rcv.at[mat * CHUNKS + k])
                avg = (recvs[mat][rows, :] + owns[mat][rows, :]) * (1.0 / REPLICAS)
                recvs[mat][rows, :] = avg
                part = avg[0:8, :] * avg[0:8, :]
                for i in range(1, heights[mat] // 8):
                    part = part + avg[8 * i:8 * i + 8, :] * avg[8 * i:8 * i + 8, :]
                sq[...] = sq[...] + part
                if mat == 1:
                    @pl.when(k >= CHUNKS - EARLY)
                    def _():
                        ag_copy(0, k - (CHUNKS - EARLY), True).start()

        partial = jnp.sum(sq1[...], keepdims=True) + jnp.sum(sq2[...], keepdims=True)
        nbuf[s] = jnp.broadcast_to(partial, (8, 128))
        norm_copies = []
        for t in range(1, STAGES):
            peer = (s + t) % STAGES
            norm_copies.append(remote(nbuf.at[s], nbuf.at[s], n_snd.at[t], n_rcv.at[s], owner_of(peer), peer))
            norm_copies[-1].start()
        for t in range(1, STAGES):
            peer = (s + t) % STAGES
            arrive(nbuf.at[peer], n_rcv.at[peer])
        total = nbuf[0]
        for t in range(1, STAGES):
            total = total + nbuf[t]
        nres[...] = total
        total_copies = [remote(nres, nres, nt_snd.at[q], nt_rcv, own_r + q * away, s) for q in range(1, REPLICAS)]
        for copy in total_copies:
            copy.start()

        chained = (s % 2 == 0) | (s == STAGES - 1)
        first = jnp.where(chained, 8 + 2 * s, CHUNKS)

        @pl.loop(EARLY, first)
        def _(k):
            ag_copy(0, k, True).start()

        @pl.when(jnp.logical_not(chained))
        def _():
            @pl.loop(0, CHUNKS)
            def _(k):
                ag_copy(1, k, True).start()

        local_copies = [pltpu.make_async_copy(recvs[mat], gouts[mat], loc.at[mat]) for mat in (0, 1)]
        for copy in local_copies:
            copy.start()

        clip = clip_of(total, maxn[...])[0:1, 0:1]
        for mat, (weights, hbm) in enumerate(((b1, (w1, m1, v1)), (b2, (w2, m2, v2)))):
            height = heights[mat]

            def fetch(k, i):
                slot = (k % SLOTS) * 3 + i
                return pltpu.make_async_copy(hbm[i].at[0, ds(k, height), :], owns[mat].at[ds(slot, height), :], st.at[mat, slot])

            for k in range(SLOTS):
                for i in range(3):
                    fetch(k, i).start()

            @pl.loop(0, CHUNKS)
            def _(k):
                for i in range(3):
                    fetch(k, i).wait()
                rows = ds(k, height)
                parts = [owns[mat][ds((k % SLOTS) * 3 + i, height), :] for i in range(3)]
                new_weight, _, _ = adamw(*parts, clip * recvs[mat][rows, :])
                weights[rows, :] = new_weight.astype(BF16)

                @pl.when(k + SLOTS < CHUNKS)
                def _():
                    for i in range(3):
                        fetch(k + SLOTS, i).start()

        @pl.when(s == 0)
        def _():
            gathered(xbuf, in_rcv)

        @pl.when(s != 0)
        def _():
            arrive(xbuf, x_rcv)

        @pl.loop(0, FF // TILE)
        def _(j):
            cols = ds(j, TILE)
            hid[:, cols] = gelu(mm(xbuf[...], b1[:, cols], NN)).astype(BF16)

        @pl.loop(0, D // TILE)
        def _(j):
            ybuf[:, ds(j, TILE)] = mm(hid[...], b2[:, ds(j, TILE)], NN).astype(BF16)

        send_x = remote(ybuf, xbuf, x_snd, x_rcv, owner_of(s + 1), (s + 1) % STAGES)

        @pl.when(s != STAGES - 1)
        def _():
            send_x.start()

        y_rows = ybuf.at[ds(r, TOK), :]

        @pl.when(s == STAGES - 1)
        def _():
            keep = pltpu.make_async_copy(y_rows, y_o, loc.at[2])
            keep.start()
            for q in range(1, REPLICAS):
                remote(ybuf.at[ds(own_r + q * away, TOK), :], y_o, y_snd.at[q + STAGES], y_rcv, own_r + q * away, s).start()
            keep.wait()
            for t in range(1, STAGES):
                remote(y_o, y_o, y_snd.at[t], y_rcv, r, (s + t) % STAGES).start()

        @pl.when(chained)
        def _():
            @pl.loop(first, CHUNKS)
            def _(k):
                ag_copy(0, k, True).start()

            @pl.loop(0, CHUNKS)
            def _(k):
                ag_copy(1, k, True).start()

        @pl.when(s == STAGES - 1)
        def _():
            for q in range(1, REPLICAS):
                remote(ybuf.at[ds(own_r + q * away, TOK), :], y_o, y_snd.at[q + STAGES], y_rcv, own_r + q * away, s).wait_send()

        @pl.when(s != 0)
        def _():
            send_g.wait_send()

        @pl.when(s != STAGES - 1)
        def _():
            send_x.wait_send()

        for copy in norm_copies + total_copies:
            copy.wait_send()
        for copy in local_copies:
            copy.wait()
        each((0, 1), lambda mat, k: ag_copy(mat, k, True).wait_send())

    nrm_o[...] = nres[...]

    @pl.when(s != STAGES - 1)
    def _():
        arrive(y_o, y_rcv)

    @pl.when(s == STAGES - 1)
    def _():
        for t in range(1, STAGES):
            remote(y_o, y_o, y_snd.at[t], y_rcv, r, (s + t) % STAGES).wait_send()


def update_kernel(nrm, maxn, *refs):
    clip = clip_of(nrm[...], maxn[...])[0:1, 0:1]
    for mat in (0, 1):
        weight, moment, sq_moment, grad = (ref[...] for ref in refs[4 * mat:4 * mat + 4])
        new = adamw(weight[0], moment[0], sq_moment[0], clip * grad)
        for ref, value in zip(refs[8 + 3 * mat:11 + 3 * mat], new):
            ref[0] = value


def solution(mesh):
    assert mesh.shape["stage"] == STAGES and mesh.shape["data"] == REPLICAS
    weight_spec = P("stage", None, None)
    acc_spec = P("data", "stage", None, None)

    def local_step(w_in, w_out, mom_in, mom_out, sq_in, sq_out, acc_in, acc_out, stage_acts, grad_y, x_next, max_norm):
        maxn = jnp.full((8, 128), max_norm, F32)
        hbm = pl.BlockSpec(memory_space=pl.ANY)
        vmem = pl.BlockSpec(memory_space=pltpu.VMEM)
        dma = pltpu.SemaphoreType.DMA
        g1, g2, nrm, y = pl.pallas_call(
            step_kernel,
            out_shape=(
                jax.ShapeDtypeStruct((D, FF), F32), jax.ShapeDtypeStruct((FF, D), F32),
                jax.ShapeDtypeStruct((8, 128), F32), jax.ShapeDtypeStruct((TOK, D), BF16),
            ),
            in_specs=[hbm] * 11 + [vmem],
            out_specs=(hbm, hbm, vmem, hbm),
            scratch_shapes=[
                pltpu.VMEM((D, FF), F32), pltpu.VMEM((FF, D), F32),
                pltpu.VMEM((D, FF), F32), pltpu.VMEM((FF, D), F32),
                pltpu.VMEM((D, FF), BF16), pltpu.VMEM((FF, D), BF16),
                pltpu.VMEM((ROWS, FF), F32), pltpu.VMEM((ROWS, FF), BF16), pltpu.VMEM((ROWS, FF), BF16),
                pltpu.VMEM((ROWS, D), BF16), pltpu.VMEM((ROWS, D), BF16), pltpu.VMEM((ROWS, D), BF16),
                pltpu.VMEM((ROWS, D), BF16), pltpu.VMEM((ROWS, D), BF16),
                pltpu.VMEM((8, FF), F32), pltpu.VMEM((8, D), F32),
                pltpu.VMEM((STAGES, 8, 128), F32), pltpu.VMEM((8, 128), F32),
                dma, dma((REPLICAS,)), dma, dma((REPLICAS,)), dma, dma, dma, dma, dma((STAGES + REPLICAS,)), dma,
                dma((2 * CHUNKS,)), dma((2 * CHUNKS,)), dma((2 * CHUNKS,)), dma((2 * CHUNKS,)),
                dma((STAGES,)), dma((STAGES,)), dma((REPLICAS,)), dma,
                dma((2, 2)), dma((2, 3 * SLOTS)), dma((3,)),
            ],
            compiler_params=pltpu.CompilerParams(has_side_effects=True, vmem_limit_bytes=67043328),
            name="reduce_backward_broadcast_forward",
        )(w_in, w_out, mom_in, mom_out, sq_in, sq_out, acc_in, acc_out, stage_acts[0], grad_y, x_next[0], maxn)

        one = pl.BlockSpec((8, 128), lambda k: (0, 0))
        wide = pl.BlockSpec((1, R1, FF), lambda k: (0, k, 0))
        tall = pl.BlockSpec((1, R2, D), lambda k: (0, k, 0))
        new = pl.pallas_call(
            update_kernel,
            grid=(CHUNKS,),
            out_shape=[jax.ShapeDtypeStruct((1, D, FF), F32)] * 3 + [jax.ShapeDtypeStruct((1, FF, D), F32)] * 3,
            in_specs=[one, one] + [wide] * 3 + [pl.BlockSpec((R1, FF), lambda k: (k, 0))] + [tall] * 3 + [pl.BlockSpec((R2, D), lambda k: (k, 0))],
            out_specs=[wide] * 3 + [tall] * 3,
            name="adamw_update",
        )(nrm, maxn, w_in, mom_in, sq_in, g1, w_out, mom_out, sq_out, g2)
        return new[0], new[3], new[1], new[4], new[2], new[5], y[None]

    in_specs = (weight_spec,) * 6 + (acc_spec, acc_spec, P("stage", "data", None), P("data", None), P(None, "data", None), P())
    out_specs = (weight_spec,) * 6 + (P(None, "data", None),)
    return jax.shard_map(local_step, mesh=mesh, in_specs=in_specs, out_specs=out_specs, check_vma=False)
```

```python
import math

import jax
import jax.numpy as jnp
from jax import lax
from jax.experimental import pallas as pl
from jax.experimental.pallas import tpu as pltpu
from jax.sharding import PartitionSpec as P

BETA_ONE = 0.9
BETA_TWO = 0.95
ADAM_EPS = 1e-8
WEIGHT_DECAY = 0.1
LR_GAIN = 0.2
CLIP_EPS = 1e-6
STEP_COUNT = 20
MESH = pl.DeviceIdType.MESH
F32, BF16 = jnp.float32, jnp.bfloat16

D, FF, STAGES, REPLICAS, TOK = 768, 3072, 8, 4, 64
ROWS = REPLICAS * TOK
CHUNKS = 48
R1, R2 = D // CHUNKS, FF // CHUNKS
UPDATES = 16
TILE = 256
SLOTS = 16
EARLY = (16, 2)
LEARN_RATE = LR_GAIN * D ** -0.5
GELU_K = math.sqrt(2.0 / math.pi)
NT = (((1,), (1,)), ((), ()))
TN = (((0,), (0,)), ((), ()))
NN = (((1,), (0,)), ((), ()))


def mm(lhs, rhs, dims):
    return lax.dot_general(lhs, rhs, dims, preferred_element_type=F32)


def gelu_parts(z):
    zz = z * z
    tanh = jnp.tanh(GELU_K * (z + 0.044715 * (zz * z)))
    cdf = 0.5 * (1.0 + tanh)
    slope = cdf + (0.5 * z) * (1.0 - tanh * tanh) * (GELU_K * (1.0 + (3 * 0.044715) * zz))
    return z * cdf, slope


def gelu(z):
    return z * (0.5 * (1.0 + jnp.tanh(GELU_K * (z + 0.044715 * (z * z * z)))))


def clip_of(sq_norm, max_norm):
    return jnp.minimum(1.0, max_norm / (jnp.sqrt(sq_norm) + CLIP_EPS))


def adamw(weight, moment, sq_moment, gradient):
    moment_new = BETA_ONE * moment + (1.0 - BETA_ONE) * gradient
    sq_new = BETA_TWO * sq_moment + (1.0 - BETA_TWO) * gradient * gradient
    step = (LEARN_RATE / (1.0 - BETA_ONE ** STEP_COUNT)) * moment_new
    v_hat = sq_new * (1.0 / (1.0 - BETA_TWO ** STEP_COUNT))
    weight_new = weight * (1.0 - LEARN_RATE * WEIGHT_DECAY) - step / (jnp.sqrt(v_hat) + ADAM_EPS)
    return weight_new, moment_new, sq_new


def owner_of(stage):
    return 3 * ((stage % 2 + (stage // 2) % 2) % 2)


def ds(index, size):
    return pl.ds(pl.multiple_of(index * size, size), size)


def step_kernel(w1, w2, m1, m2, v1, v2, acc1, acc2, a_in, gy_in, x_in, maxn,
                g1_o, g2_o, nrm_o, y_o,
                recv1, recv2, own1, own2, b1, b2, gp, hid, dz, abuf, gbuf, gnext, xbuf, ybuf, sq1, sq2, nbuf, nplane,
                a_snd, a_rcv, in_snd, in_rcv, g_snd, g_rcv, x_snd, x_rcv, y_snd, y_rcv, rs_snd, rs_rcv, ag_snd, ag_rcv,
                n_snd, n_rcv, np_snd, np_rcv, nt_snd, nt_rcv, ld, st, loc):
    r = lax.axis_index("data")
    s = lax.axis_index("stage")
    own_r = owner_of(s)
    away = 1 - 2 * (own_r // 3)
    d = (r - own_r) * away
    partner = s + 1 - 2 * (s % 2)
    pair, plane = s // 2, r // 3
    early = EARLY[0] + (EARLY[1] - EARLY[0]) * (s % 2)
    accs, recvs, owns, gouts = (acc1, acc2), (recv1, recv2), (own1, own2), (g1_o, g2_o)
    heights = (R1, R2)

    def remote(src, dst, snd, rcv, to_r, to_s):
        return pltpu.make_async_remote_copy(src_ref=src, dst_ref=dst, send_sem=snd, recv_sem=rcv,
                                            device_id=(to_r, to_s), device_id_type=MESH)

    def arrive(ref, sem):
        pltpu.make_async_copy(ref, ref, sem).wait()

    def gather(src, dst, snd, rcv):
        part = dst.at[ds(r, TOK), :]

        @pl.when(d == 0)
        def _():
            pltpu.make_async_copy(src, part, rcv.at[r]).start()

        @pl.when(d != 0)
        def _():
            remote(src, part, snd, rcv.at[r], own_r, s).start()

    def gathered(dst, rcv):
        for q in range(REPLICAS):
            arrive(dst.at[pl.ds(q * TOK, TOK), :], rcv.at[q])

    barrier = pltpu.get_barrier_semaphore()
    for q in range(1, REPLICAS):
        pl.semaphore_signal(barrier, inc=1, device_id=((r + q) % REPLICAS, s), device_id_type=MESH)

    @pl.when(d == 0)
    def _():
        for t in range(1, STAGES):
            peer = (s + t) % STAGES
            pl.semaphore_signal(barrier, inc=1, device_id=(owner_of(peer), peer), device_id_type=MESH)

    @pl.when(s != STAGES - 1)
    def _():
        pl.semaphore_signal(barrier, inc=1, device_id=(r, STAGES - 1), device_id_type=MESH)

    at_end = (r == 0) | (r == REPLICAS - 1)

    @pl.when(at_end)
    def _():
        pl.semaphore_signal(barrier, inc=1, device_id=(r, partner), device_id_type=MESH)

    signals = REPLICAS - 1 + jnp.where(at_end, 1, 0) + jnp.where(d == 0, STAGES - 1, 0) + jnp.where(s == STAGES - 1, STAGES - 1, 0)
    pl.semaphore_wait(barrier, signals)

    @pl.when(s == STAGES - 1)
    def _():
        gather(gy_in, gbuf, in_snd, in_rcv)

    gather(a_in, abuf, a_snd, a_rcv)

    @pl.when(s == 0)
    def _():
        gather(x_in, xbuf, in_snd, in_rcv)

    def rs_copy(mat, k, src):
        part = recvs[mat].at[ds(k, heights[mat]), :]
        sem = mat * CHUNKS + k
        return remote(src, part, rs_snd.at[sem], rs_rcv.at[sem], r - away, s)

    def rs_src(mat, k):
        return owns[mat].at[ds(k, heights[mat]), :]

    def ag_copy(mat, k, from_vmem):
        rows = ds(k, heights[mat])
        src = recvs[mat] if from_vmem else gouts[mat]
        sem = mat * CHUNKS + k
        return remote(src.at[rows, :], gouts[mat].at[rows, :], ag_snd.at[sem], ag_rcv.at[sem], r + away, s)

    def ag_range(lo, hi):
        for mat in (0, 1):
            @pl.loop(jnp.clip(lo - mat * CHUNKS, 0, CHUNKS), jnp.clip(hi - mat * CHUNKS, 0, CHUNKS))
            def _(k):
                ag_copy(mat, k, True).start()

    def each(mats, fn, lo=0, hi=CHUNKS):
        for mat in mats:
            @pl.loop(lo, hi)
            def _(k):
                fn(mat, k)

    @pl.when(d == 3)
    def _():
        parts = 4
        loads = [pltpu.make_async_copy(acc1.at[0, 0, pl.ds(q * D // parts, D // parts), :], own1.at[pl.ds(q * D // parts, D // parts), :], ld.at[0, q])
                 for q in range(parts)]
        loads.append(pltpu.make_async_copy(acc2.at[0, 0], own2, ld.at[1, 0]))
        for copy in loads:
            copy.start()
        for q in range(parts):
            loads[q].wait()
            each((0,), lambda mat, k: rs_copy(mat, k, rs_src(mat, k)).start(), q * CHUNKS // parts, (q + 1) * CHUNKS // parts)
        loads[parts].wait()
        each((1,), lambda mat, k: rs_copy(mat, k, rs_src(mat, k)).start())

    @pl.when((d == 1) | (d == 2))
    def _():
        own_copies = [pltpu.make_async_copy(accs[mat].at[0, 0], owns[mat], ld.at[mat, 0]) for mat in (0, 1)]
        for copy in own_copies:
            copy.start()
        for mat in (0, 1):
            own_copies[mat].wait()

            @pl.loop(0, CHUNKS)
            def _(k):
                rows = ds(k, heights[mat])
                arrive(recvs[mat].at[rows, :], rs_rcv.at[mat * CHUNKS + k])
                recvs[mat][rows, :] = recvs[mat][rows, :] + owns[mat][rows, :]
                rs_copy(mat, k, recvs[mat].at[rows, :]).start()

    @pl.when(d == 3)
    def _():
        arrive(nplane.at[plane], np_rcv.at[0])
        remote(nplane.at[plane], nplane.at[plane], np_snd.at[0], np_rcv.at[1], own_r, s).start()
        arrive(nplane.at[1 - plane], np_rcv.at[2])
        for q in (1, 2):
            remote(nplane, nplane, nt_snd.at[q], nt_rcv, own_r + q * away, s).start()

    @pl.when(d != 0)
    def _():
        for mat in (0, 1):
            @pl.loop(0, CHUNKS)
            def _(k):
                rows = ds(k, heights[mat])
                arrive(gouts[mat].at[rows, :], ag_rcv.at[mat * CHUNKS + k])

                @pl.when(d != 3)
                def _():
                    ag_copy(mat, k, False).start()

                if mat == 1:
                    @pl.when((s == STAGES - 1) & (k == CHUNKS - 8))
                    def _():
                        arrive(y_o, y_rcv)
                        for t in range(1, STAGES):
                            remote(y_o, y_o, y_snd.at[t], y_rcv, r, (s + t) % STAGES).start()

        @pl.when(d != 3)
        def _():
            arrive(nplane, nt_rcv)

        @pl.when(d == 3)
        def _():
            remote(nplane.at[plane], nplane.at[plane], np_snd.at[0], np_rcv.at[1], own_r, s).wait_send()
            for q in (1, 2):
                remote(nplane, nplane, nt_snd.at[q], nt_rcv, own_r + q * away, s).wait_send()

        remote(a_in, abuf.at[ds(r, TOK), :], a_snd, a_rcv.at[r], own_r, s).wait_send()

        @pl.when((s == 0) | (s == STAGES - 1))
        def _():
            remote(x_in, xbuf.at[ds(r, TOK), :], in_snd, in_rcv.at[r], own_r, s).wait_send()

        each((0, 1), lambda mat, k: rs_copy(mat, k, rs_src(mat, k)).wait_send())

        @pl.when(d != 3)
        def _():
            each((0, 1), lambda mat, k: ag_copy(mat, k, False).wait_send())

    @pl.when(d == 0)
    def _():
        loads = [pltpu.make_async_copy(w.at[0], own, ld.at[mat, 0]) for mat, (w, own) in enumerate(((w1, own1), (w2, own2)))]
        for copy in loads:
            copy.start()
        sq1[...] = jnp.zeros_like(sq1)
        sq2[...] = jnp.zeros_like(sq2)
        loads[0].wait()

        @pl.loop(0, CHUNKS)
        def _(k):
            b1[ds(k, R1), :] = own1[ds(k, R1), :].astype(BF16)

        loads[1].wait()

        @pl.loop(0, CHUNKS)
        def _(k):
            b2[ds(k, R2), :] = own2[ds(k, R2), :].astype(BF16)

        own_copies = [pltpu.make_async_copy(accs[mat].at[0, 0], owns[mat], ld.at[mat, 1]) for mat in (0, 1)]
        for copy in own_copies:
            copy.start()

        gathered(abuf, a_rcv)

        @pl.loop(0, FF // TILE)
        def _(j):
            cols = ds(j, TILE)
            value, slope = gelu_parts(mm(abuf[...], b1[:, cols], NN))
            hid[:, cols] = value.astype(BF16)
            gp[:, cols] = slope

        @pl.when(s == STAGES - 1)
        def _():
            gathered(gbuf, in_rcv)

        @pl.when(s != STAGES - 1)
        def _():
            arrive(gbuf, g_rcv)

        @pl.loop(0, FF // TILE)
        def _(j):
            cols = ds(j, TILE)
            dz[:, cols] = (gp[:, cols] * mm(gbuf[...], b2[cols, :], NT)).astype(BF16)

        send_g = remote(gnext, gbuf, g_snd, g_rcv, owner_of(s + STAGES - 1), (s + STAGES - 1) % STAGES)

        @pl.when(s != 0)
        def _():
            @pl.loop(0, D // TILE)
            def _(j):
                gnext[:, ds(j, TILE)] = mm(dz[...], b1[ds(j, TILE), :], NT).astype(BF16)

            send_g.start()

        own_copies[0].wait()

        @pl.loop(0, FF // TILE)
        def _(j):
            cols = ds(j, TILE)
            own1[:, cols] = own1[:, cols] + mm(abuf[...], dz[:, cols], TN)

        own_copies[1].wait()

        @pl.loop(0, FF // TILE)
        def _(j):
            cols = ds(j, TILE)
            own2[cols, :] = own2[cols, :] + mm(hid[:, cols], gbuf[...], TN)

        for mat in (0, 1):
            sq = (sq1, sq2)[mat]

            @pl.loop(0, CHUNKS)
            def _(k):
                rows = ds(k, heights[mat])
                arrive(recvs[mat].at[rows, :], rs_rcv.at[mat * CHUNKS + k])
                avg = (recvs[mat][rows, :] + owns[mat][rows, :]) * (1.0 / REPLICAS)
                recvs[mat][rows, :] = avg
                part = avg[0:8, :] * avg[0:8, :]
                for i in range(1, heights[mat] // 8):
                    part = part + avg[8 * i:8 * i + 8, :] * avg[8 * i:8 * i + 8, :]
                sq[...] = sq[...] + part
                if mat == 1:
                    @pl.when(k >= CHUNKS - early)
                    def _():
                        ag_copy(0, k - (CHUNKS - early), True).start()

        chained = (s % 2 == 0) | (s == STAGES - 1)
        first = jnp.where(chained, 34 + 6 * s - 6 * (s // 7), 2 * CHUNKS)
        second = jnp.where(chained, first + 3, 2 * CHUNKS)
        ag_range(early, first)

        partial = jnp.sum(sq1[...], keepdims=True) + jnp.sum(sq2[...], keepdims=True)
        nbuf[pair] = jnp.broadcast_to(partial, (8, 128))
        norm_copies = []
        for q in range(1, REPLICAS):
            other = (pair + q) % REPLICAS
            norm_copies.append(remote(nbuf.at[pair], nbuf.at[pair], n_snd.at[q], n_rcv.at[pair], r, 2 * other + (other + plane) % 2))
            norm_copies[-1].start()
        for q in range(1, REPLICAS):
            other = (pair + q) % REPLICAS
            arrive(nbuf.at[other], n_rcv.at[other])
        nplane[plane] = (nbuf[0] + nbuf[1]) + (nbuf[2] + nbuf[3])
        norm_copies.append(remote(nplane.at[plane], nplane.at[plane], np_snd.at[0], np_rcv.at[0], r, partner))
        norm_copies[-1].start()
        arrive(nplane.at[1 - plane], np_rcv.at[1])
        norm_copies.append(remote(nplane.at[1 - plane], nplane.at[1 - plane], np_snd.at[1], np_rcv.at[2], r, partner))
        norm_copies[-1].start()
        total = nplane[0] + nplane[1]

        local_copies = [pltpu.make_async_copy(recvs[mat], gouts[mat], loc.at[mat]) for mat in (0, 1)]
        for copy in local_copies:
            copy.start()

        clip = clip_of(total, maxn[...])[0:1, 0:1]
        for mat, (weights, hbm) in enumerate(((b1, (w1, m1, v1)), (b2, (w2, m2, v2)))):
            height = heights[mat]

            def fetch(k, i):
                slot = (k % SLOTS) * 3 + i
                return pltpu.make_async_copy(hbm[i].at[0, ds(k, height), :], owns[mat].at[ds(slot, height), :], st.at[mat, slot])

            for k in range(SLOTS):
                for i in range(3):
                    fetch(k, i).start()

            @pl.loop(0, CHUNKS)
            def _(k):
                for i in range(3):
                    fetch(k, i).wait()
                rows = ds(k, height)
                parts = [owns[mat][ds((k % SLOTS) * 3 + i, height), :] for i in range(3)]
                new_weight, _, _ = adamw(*parts, clip * recvs[mat][rows, :])
                weights[rows, :] = new_weight.astype(BF16)

                @pl.when(k + SLOTS < CHUNKS)
                def _():
                    for i in range(3):
                        fetch(k + SLOTS, i).start()

        @pl.when(s == 0)
        def _():
            gathered(xbuf, in_rcv)

        @pl.when(s != 0)
        def _():
            arrive(xbuf, x_rcv)

        ag_range(first, second)

        @pl.loop(0, FF // TILE)
        def _(j):
            cols = ds(j, TILE)
            hid[:, cols] = gelu(mm(xbuf[...], b1[:, cols], NN)).astype(BF16)

        @pl.loop(0, D // TILE)
        def _(j):
            ybuf[:, ds(j, TILE)] = mm(hid[...], b2[:, ds(j, TILE)], NN).astype(BF16)

        send_x = remote(ybuf, xbuf, x_snd, x_rcv, owner_of(s + 1), (s + 1) % STAGES)

        @pl.when(s != STAGES - 1)
        def _():
            send_x.start()

        y_rows = ybuf.at[ds(r, TOK), :]

        @pl.when(s == STAGES - 1)
        def _():
            keep = pltpu.make_async_copy(y_rows, y_o, loc.at[2])
            keep.start()
            for q in range(1, REPLICAS):
                remote(ybuf.at[ds(own_r + q * away, TOK), :], y_o, y_snd.at[q + STAGES], y_rcv, own_r + q * away, s).start()
            keep.wait()
            for t in range(1, STAGES):
                remote(y_o, y_o, y_snd.at[t], y_rcv, r, (s + t) % STAGES).start()

        ag_range(second, 2 * CHUNKS)

        @pl.when(s == STAGES - 1)
        def _():
            for q in range(1, REPLICAS):
                remote(ybuf.at[ds(own_r + q * away, TOK), :], y_o, y_snd.at[q + STAGES], y_rcv, own_r + q * away, s).wait_send()

        @pl.when(s != 0)
        def _():
            send_g.wait_send()

        @pl.when(s != STAGES - 1)
        def _():
            send_x.wait_send()

        for copy in norm_copies:
            copy.wait_send()
        for copy in local_copies:
            copy.wait()
        each((0, 1), lambda mat, k: ag_copy(mat, k, True).wait_send())

    nrm_o[...] = nplane[0] + nplane[1]

    @pl.when(s != STAGES - 1)
    def _():
        arrive(y_o, y_rcv)

    @pl.when(s == STAGES - 1)
    def _():
        for t in range(1, STAGES):
            remote(y_o, y_o, y_snd.at[t], y_rcv, r, (s + t) % STAGES).wait_send()


def update_kernel(nrm, maxn, *refs):
    clip = clip_of(nrm[...], maxn[...])[0:1, 0:1]
    for mat in (0, 1):
        weight, moment, sq_moment, grad = (ref[...] for ref in refs[4 * mat:4 * mat + 4])
        new = adamw(weight[0], moment[0], sq_moment[0], clip * grad)
        for ref, value in zip(refs[8 + 3 * mat:11 + 3 * mat], new):
            ref[0] = value


def solution(mesh):
    assert mesh.shape["stage"] == STAGES and mesh.shape["data"] == REPLICAS
    weight_spec = P("stage", None, None)
    acc_spec = P("data", "stage", None, None)

    def local_step(w_in, w_out, mom_in, mom_out, sq_in, sq_out, acc_in, acc_out, stage_acts, grad_y, x_next, max_norm):
        maxn = jnp.full((8, 128), max_norm, F32)
        hbm = pl.BlockSpec(memory_space=pl.ANY)
        vmem = pl.BlockSpec(memory_space=pltpu.VMEM)
        dma = pltpu.SemaphoreType.DMA
        g1, g2, nrm, y = pl.pallas_call(
            step_kernel,
            out_shape=(
                jax.ShapeDtypeStruct((D, FF), F32), jax.ShapeDtypeStruct((FF, D), F32),
                jax.ShapeDtypeStruct((8, 128), F32), jax.ShapeDtypeStruct((TOK, D), BF16),
            ),
            in_specs=[hbm] * 11 + [vmem],
            out_specs=(hbm, hbm, vmem, hbm),
            scratch_shapes=[
                pltpu.VMEM((D, FF), F32), pltpu.VMEM((FF, D), F32),
                pltpu.VMEM((D, FF), F32), pltpu.VMEM((FF, D), F32),
                pltpu.VMEM((D, FF), BF16), pltpu.VMEM((FF, D), BF16),
                pltpu.VMEM((ROWS, FF), F32), pltpu.VMEM((ROWS, FF), BF16), pltpu.VMEM((ROWS, FF), BF16),
                pltpu.VMEM((ROWS, D), BF16), pltpu.VMEM((ROWS, D), BF16), pltpu.VMEM((ROWS, D), BF16),
                pltpu.VMEM((ROWS, D), BF16), pltpu.VMEM((ROWS, D), BF16),
                pltpu.VMEM((8, FF), F32), pltpu.VMEM((8, D), F32),
                pltpu.VMEM((REPLICAS, 8, 128), F32), pltpu.VMEM((2, 8, 128), F32),
                dma, dma((REPLICAS,)), dma, dma((REPLICAS,)), dma, dma, dma, dma, dma((STAGES + REPLICAS,)), dma,
                dma((2 * CHUNKS,)), dma((2 * CHUNKS,)), dma((2 * CHUNKS,)), dma((2 * CHUNKS,)),
                dma((REPLICAS,)), dma((REPLICAS,)), dma((2,)), dma((3,)), dma((REPLICAS,)), dma,
                dma((2, 4)), dma((2, 3 * SLOTS)), dma((3,)),
            ],
            compiler_params=pltpu.CompilerParams(has_side_effects=True, collective_id=0, vmem_limit_bytes=67043328),
            name="reduce_backward_broadcast_forward",
        )(w_in, w_out, mom_in, mom_out, sq_in, sq_out, acc_in, acc_out, stage_acts[0], grad_y, x_next[0], maxn)

        one = pl.BlockSpec((8, 128), lambda k: (0, 0))
        short, high = D // UPDATES, FF // UPDATES
        wide = pl.BlockSpec((1, short, FF), lambda k: (0, k, 0))
        tall = pl.BlockSpec((1, high, D), lambda k: (0, k, 0))
        new = pl.pallas_call(
            update_kernel,
            grid=(UPDATES,),
            out_shape=[jax.ShapeDtypeStruct((1, D, FF), F32)] * 3 + [jax.ShapeDtypeStruct((1, FF, D), F32)] * 3,
            in_specs=[one, one] + [wide] * 3 + [pl.BlockSpec((short, FF), lambda k: (k, 0))] + [tall] * 3 + [pl.BlockSpec((high, D), lambda k: (k, 0))],
            out_specs=[wide] * 3 + [tall] * 3,
            name="adamw_update",
        )(nrm, maxn, w_in, mom_in, sq_in, g1, w_out, mom_out, sq_out, g2)
        return new[0], new[3], new[1], new[4], new[2], new[5], y[None]

    in_specs = (weight_spec,) * 6 + (acc_spec, acc_spec, P("stage", "data", None), P("data", None), P(None, "data", None), P())
    out_specs = (weight_spec,) * 6 + (P(None, "data", None),)
    return jax.shard_map(local_step, mesh=mesh, in_specs=in_specs, out_specs=out_specs, check_vma=False)
```

```python
import math

import jax
import jax.numpy as jnp
from jax import lax
from jax.experimental import pallas as pl
from jax.experimental.pallas import tpu as pltpu
from jax.sharding import PartitionSpec as P

BETA_ONE = 0.9
BETA_TWO = 0.95
ADAM_EPS = 1e-8
WEIGHT_DECAY = 0.1
LR_GAIN = 0.2
CLIP_EPS = 1e-6
STEP_COUNT = 20
MESH = pl.DeviceIdType.MESH
F32, BF16 = jnp.float32, jnp.bfloat16

D, FF, STAGES, REPLICAS, TOK = 768, 3072, 8, 4, 64
ROWS = REPLICAS * TOK
CHUNKS = 48
R1, R2 = D // CHUNKS, FF // CHUNKS
LAG = 16
TILE = 256
SLOTS = 8
EARLY = (9, 4)
VMEM_LIMIT = 19800000
FLUSH = 4
LEARN_RATE = LR_GAIN * D ** -0.5
GELU_K = math.sqrt(2.0 / math.pi)
NT = (((1,), (1,)), ((), ()))
TN = (((0,), (0,)), ((), ()))
NN = (((1,), (0,)), ((), ()))


def mm(lhs, rhs, dims):
    return lax.dot_general(lhs, rhs, dims, preferred_element_type=F32)


def gelu_parts(z):
    zz = z * z
    tanh = jnp.tanh(GELU_K * (z + 0.044715 * (zz * z)))
    cdf = 0.5 * (1.0 + tanh)
    slope = cdf + (0.5 * z) * (1.0 - tanh * tanh) * (GELU_K * (1.0 + (3 * 0.044715) * zz))
    return z * cdf, slope


def gelu(z):
    return z * (0.5 * (1.0 + jnp.tanh(GELU_K * (z + 0.044715 * (z * z * z)))))


def clip_of(sq_norm, max_norm):
    return jnp.minimum(1.0, max_norm / (jnp.sqrt(sq_norm) + CLIP_EPS))


def moments(moment, sq_moment, gradient):
    return BETA_ONE * moment + (1.0 - BETA_ONE) * gradient, BETA_TWO * sq_moment + (1.0 - BETA_TWO) * gradient * gradient


def new_weight(weight, moment_new, sq_new):
    step = (LEARN_RATE / (1.0 - BETA_ONE ** STEP_COUNT)) * moment_new
    v_hat = sq_new * (1.0 / (1.0 - BETA_TWO ** STEP_COUNT))
    return weight * (1.0 - LEARN_RATE * WEIGHT_DECAY) - step / (jnp.sqrt(v_hat) + ADAM_EPS)


def owner_of(stage):
    return 3 * ((stage % 2 + (stage // 2) % 2) % 2)


def ds(index, size):
    return pl.ds(pl.multiple_of(index * size, size), size)


def step_kernel(w1, w2, m1, m2, v1, v2, acc1, acc2, a_in, gy_in, x_in, maxn,
                recv1, recv2, own1, own2, sq_o, v2_o, g1_o, g2_o, y_o,
                b1, b2, hid, ring1, ring2, ringv, abuf, gbuf, gnext, xbuf, ybuf, sq1, sq2, nbuf, nplane,
                a_snd, a_rcv, in_snd, in_rcv, g_snd, g_rcv, x_snd, x_rcv, y_snd, y_rcv, rs_snd, rs_rcv, ag_snd, ag_rcv,
                n_snd, n_rcv, np_snd, np_rcv, nt_snd, nt_rcv, ld, st, vo, loc):
    r = lax.axis_index("data")
    s = lax.axis_index("stage")
    own_r = owner_of(s)
    away = 1 - 2 * (own_r // 3)
    d = (r - own_r) * away
    partner = s + 1 - 2 * (s % 2)
    pair, plane = s // 2, r // 3
    early = EARLY[0] + (EARLY[1] - EARLY[0]) * (s % 2)
    accs, recvs, owns, gouts = (acc1, acc2), (recv1, recv2), (own1, own2), (g1_o, g2_o)
    rings, weights_hbm, moments_hbm = (ring1, ring2), (w1, w2), (m1, m2)
    heights = (R1, R2)
    gp, dz = sq_o.at[pl.ds(0, ROWS), :], sq_o.at[pl.ds(ROWS, ROWS), :]

    def remote(src, dst, snd, rcv, to_r, to_s):
        return pltpu.make_async_remote_copy(src_ref=src, dst_ref=dst, send_sem=snd, recv_sem=rcv,
                                            device_id=(to_r, to_s), device_id_type=MESH)

    def arrive(ref, sem):
        pltpu.make_async_copy(ref, ref, sem).wait()

    def gather(src, dst, snd, rcv):
        part = dst.at[ds(r, TOK), :]

        @pl.when(d == 0)
        def _():
            pltpu.make_async_copy(src, part, rcv.at[r]).start()

        @pl.when(d != 0)
        def _():
            remote(src, part, snd, rcv.at[r], own_r, s).start()

    def gathered(dst, rcv):
        for q in range(REPLICAS):
            arrive(dst.at[pl.ds(q * TOK, TOK), :], rcv.at[q])

    barrier = pltpu.get_barrier_semaphore()
    for q in range(1, REPLICAS):
        pl.semaphore_signal(barrier, inc=1, device_id=((r + q) % REPLICAS, s), device_id_type=MESH)

    @pl.when(d == 0)
    def _():
        for t in range(1, STAGES):
            peer = (s + t) % STAGES
            pl.semaphore_signal(barrier, inc=1, device_id=(owner_of(peer), peer), device_id_type=MESH)

    @pl.when(s != STAGES - 1)
    def _():
        pl.semaphore_signal(barrier, inc=1, device_id=(r, STAGES - 1), device_id_type=MESH)

    at_end = (r == 0) | (r == REPLICAS - 1)

    @pl.when(at_end)
    def _():
        pl.semaphore_signal(barrier, inc=1, device_id=(r, partner), device_id_type=MESH)

    signals = REPLICAS - 1 + jnp.where(at_end, 1, 0) + jnp.where(d == 0, STAGES - 1, 0) + jnp.where(s == STAGES - 1, STAGES - 1, 0)
    pl.semaphore_wait(barrier, signals)

    @pl.when(s == STAGES - 1)
    def _():
        gather(gy_in, gbuf, in_snd, in_rcv)

    gather(a_in, abuf, a_snd, a_rcv)

    @pl.when(s == 0)
    def _():
        gather(x_in, xbuf, in_snd, in_rcv)

    def rs_copy(mat, k, src):
        part = recvs[mat].at[ds(k, heights[mat]), :]
        sem = mat * CHUNKS + k
        return remote(src, part, rs_snd.at[sem], rs_rcv.at[sem], r - away, s)

    def rs_src(mat, k):
        return owns[mat].at[ds(k, heights[mat]), :]

    def ag_copy(mat, k, from_vmem):
        rows = ds(k, heights[mat])
        src = recvs[mat] if from_vmem else gouts[mat]
        sem = mat * CHUNKS + k
        return remote(src.at[rows, :], gouts[mat].at[rows, :], ag_snd.at[sem], ag_rcv.at[sem], r + away, s)

    def ag_range(lo, hi):
        for mat in (0, 1):
            @pl.loop(jnp.clip(lo - mat * CHUNKS, 0, CHUNKS), jnp.clip(hi - mat * CHUNKS, 0, CHUNKS))
            def _(k):
                ag_copy(mat, k, True).start()

    def each(mats, fn, lo=0, hi=CHUNKS):
        for mat in mats:
            @pl.loop(lo, hi)
            def _(k):
                fn(mat, k)

    @pl.when(d == 3)
    def _():
        parts = 4
        loads = [pltpu.make_async_copy(acc1.at[0, 0, pl.ds(q * D // parts, D // parts), :], own1.at[pl.ds(q * D // parts, D // parts), :], ld.at[0, q])
                 for q in range(parts)]
        loads.append(pltpu.make_async_copy(acc2.at[0, 0], own2, ld.at[1, 0]))
        for copy in loads:
            copy.start()
        for q in range(parts):
            loads[q].wait()
            each((0,), lambda mat, k: rs_copy(mat, k, rs_src(mat, k)).start(), q * CHUNKS // parts, (q + 1) * CHUNKS // parts)
        loads[parts].wait()
        each((1,), lambda mat, k: rs_copy(mat, k, rs_src(mat, k)).start())

    @pl.when((d == 1) | (d == 2))
    def _():
        own_copies = [pltpu.make_async_copy(accs[mat].at[0, 0], owns[mat], ld.at[mat, 0]) for mat in (0, 1)]
        for copy in own_copies:
            copy.start()
        for mat in (0, 1):
            own_copies[mat].wait()

            @pl.loop(0, CHUNKS)
            def _(k):
                rows = ds(k, heights[mat])
                arrive(recvs[mat].at[rows, :], rs_rcv.at[mat * CHUNKS + k])
                recvs[mat][rows, :] = recvs[mat][rows, :] + owns[mat][rows, :]
                rs_copy(mat, k, recvs[mat].at[rows, :]).start()

    def load(mat, k, src, ring, sem):
        slot = k % SLOTS
        return pltpu.make_async_copy(src, ring.at[slot], st.at[sem * SLOTS + slot])

    def load_rows(mat, k, hbm):
        return load(mat, k, hbm.at[ds(k, heights[mat]), :], rings[mat], mat)

    def load_v2(k, hbm):
        return load(1, k, hbm.at[ds(k, R2), :], ringv, 2)

    def store_v2(k):
        return pltpu.make_async_copy(ringv.at[k % SLOTS], v2_o.at[ds(k, R2), :], vo.at[k % SLOTS])

    def whole(mat, src, dst, sem):
        return pltpu.make_async_copy(src.at[0], dst, ld.at[mat, sem])

    @pl.when(d != 0)
    def _():
        fills = ([whole(0, w1, recv1, 0), whole(0, m1, own1, 1), whole(0, v1, sq_o, 2)], [whole(1, w2, recv2, 0), whole(1, m2, own2, 1)])

        def prefetch():
            each((0, 1), lambda mat, k: rs_copy(mat, k, rs_src(mat, k)).wait_send())
            for copy in fills[0] + fills[1]:
                copy.start()

        def pass_on(mat, k):
            rows = ds(k, heights[mat])
            arrive(gouts[mat].at[rows, :], ag_rcv.at[mat * CHUNKS + k])

            @pl.when(d != 3)
            def _():
                ag_copy(mat, k, False).start()

        @pl.when(d == 3)
        def _():
            prefetch()
            arrive(nplane.at[plane], np_rcv.at[0])
            remote(nplane.at[plane], nplane.at[plane], np_snd.at[0], np_rcv.at[1], own_r, s).start()
            arrive(nplane.at[1 - plane], np_rcv.at[2])
            for q in (1, 2):
                remote(nplane, nplane, nt_snd.at[q], nt_rcv, own_r + q * away, s).start()

        each((0,), pass_on, 0, LAG // 2)

        @pl.when(d != 3)
        def _():
            prefetch()

        each((0,), pass_on, LAG // 2, LAG)

        @pl.when(d != 3)
        def _():
            arrive(nplane, nt_rcv)

        clip = clip_of(nplane[0] + nplane[1], maxn[...])[0:1, 0:1]
        for copy in fills[0]:
            copy.wait()

        def update_first(k):
            load_rows(0, k, g1_o).wait()
            rows = ds(k, R1)
            moment, sq_moment = moments(own1[rows, :], sq_o[rows, :], clip * ring1[k % SLOTS])
            recv1[rows, :] = new_weight(recv1[rows, :], moment, sq_moment)
            own1[rows, :] = moment
            sq_o[rows, :] = sq_moment

        def update_second(k):
            load_rows(1, k, g2_o).wait()
            load_v2(k, v2.at[0]).wait()
            rows = ds(k, R2)
            moment, sq_moment = moments(own2[rows, :], ringv[k % SLOTS], clip * ring2[k % SLOTS])
            recv2[rows, :] = new_weight(recv2[rows, :], moment, sq_moment)
            own2[rows, :] = moment
            ringv[k % SLOTS] = sq_moment
            store_v2(k).start()

        @pl.loop(LAG, 2 * LAG)
        def _(k):
            pass_on(0, k)
            for i in (0, 1):
                load_rows(0, 2 * (k - LAG) + i, g1_o).start()

            @pl.when(k > LAG)
            def _():
                for i in (0, 1):
                    update_first(2 * (k - LAG - 1) + i)

        update_first(2 * LAG - 2)

        @pl.loop(2 * LAG, CHUNKS)
        def _(k):
            pass_on(0, k)
            load_rows(0, k, g1_o).start()
            update_first(k - 1)

        update_first(CHUNKS - 1)
        for copy in fills[1]:
            copy.wait()

        @pl.loop(0, CHUNKS)
        def _(k):
            pass_on(1, k)

            @pl.when(k >= SLOTS)
            def _():
                store_v2(k - SLOTS).wait()

            load_rows(1, k, g2_o).start()
            load_v2(k, v2.at[0]).start()

            @pl.when(k > 0)
            def _():
                update_second(k - 1)

            @pl.when((s == STAGES - 1) & (k == CHUNKS - 8))
            def _():
                arrive(y_o, y_rcv)
                for t in range(1, STAGES):
                    remote(y_o, y_o, y_snd.at[t], y_rcv, r, (s + t) % STAGES).start()

        update_second(CHUNKS - 1)
        each((1,), lambda mat, k: store_v2(k).wait(), CHUNKS - SLOTS, CHUNKS)

        @pl.when(d == 3)
        def _():
            remote(nplane.at[plane], nplane.at[plane], np_snd.at[0], np_rcv.at[1], own_r, s).wait_send()
            for q in (1, 2):
                remote(nplane, nplane, nt_snd.at[q], nt_rcv, own_r + q * away, s).wait_send()

        remote(a_in, abuf.at[ds(r, TOK), :], a_snd, a_rcv.at[r], own_r, s).wait_send()

        @pl.when((s == 0) | (s == STAGES - 1))
        def _():
            remote(x_in, xbuf.at[ds(r, TOK), :], in_snd, in_rcv.at[r], own_r, s).wait_send()

        @pl.when(d != 3)
        def _():
            each((0, 1), lambda mat, k: ag_copy(mat, k, False).wait_send())

    @pl.when(d == 0)
    def _():
        loads = [pltpu.make_async_copy(w.at[0], own, ld.at[mat, 0]) for mat, (w, own) in enumerate(((w1, own1), (w2, own2)))]
        for copy in loads:
            copy.start()
        sq1[...] = jnp.zeros_like(sq1)
        sq2[...] = jnp.zeros_like(sq2)
        loads[0].wait()

        @pl.loop(0, CHUNKS)
        def _(k):
            b1[ds(k, R1), :] = own1[ds(k, R1), :].astype(BF16)

        loads[1].wait()

        @pl.loop(0, CHUNKS)
        def _(k):
            b2[ds(k, R2), :] = own2[ds(k, R2), :].astype(BF16)

        own_copies = [pltpu.make_async_copy(accs[mat].at[0, 0], owns[mat], ld.at[mat, 1]) for mat in (0, 1)]
        for copy in own_copies:
            copy.start()

        gathered(abuf, a_rcv)

        @pl.loop(0, FF // TILE)
        def _(j):
            cols = ds(j, TILE)
            value, slope = gelu_parts(mm(abuf[...], b1[:, cols], NN))
            hid[:, cols] = value.astype(BF16)
            gp[:, cols] = slope

        @pl.when(s == STAGES - 1)
        def _():
            gathered(gbuf, in_rcv)

        @pl.when(s != STAGES - 1)
        def _():
            arrive(gbuf, g_rcv)

        @pl.loop(0, FF // TILE)
        def _(j):
            cols = ds(j, TILE)
            dz[:, cols] = (gp[:, cols] * mm(gbuf[...], b2[cols, :], NT)).astype(BF16).astype(F32)

        send_g = remote(gnext, gbuf, g_snd, g_rcv, owner_of(s + STAGES - 1), (s + STAGES - 1) % STAGES)

        @pl.when(s != 0)
        def _():
            @pl.loop(0, D // TILE)
            def _(j):
                gnext[:, ds(j, TILE)] = mm(dz[...].astype(BF16), b1[ds(j, TILE), :], NT).astype(BF16)

            send_g.start()

        own_copies[0].wait()

        @pl.loop(0, FF // TILE)
        def _(j):
            cols = ds(j, TILE)
            own1[:, cols] = own1[:, cols] + mm(abuf[...], dz[:, cols].astype(BF16), TN)

        own_copies[1].wait()

        @pl.loop(0, FF // TILE)
        def _(j):
            cols = ds(j, TILE)
            own2[cols, :] = own2[cols, :] + mm(hid[:, cols], gbuf[...], TN)

        for mat in (0, 1):
            sq = (sq1, sq2)[mat]

            @pl.loop(0, CHUNKS)
            def _(k):
                rows = ds(k, heights[mat])
                arrive(recvs[mat].at[rows, :], rs_rcv.at[mat * CHUNKS + k])
                avg = (recvs[mat][rows, :] + owns[mat][rows, :]) * (1.0 / REPLICAS)
                recvs[mat][rows, :] = avg
                part = avg[0:8, :] * avg[0:8, :]
                for i in range(1, heights[mat] // 8):
                    part = part + avg[8 * i:8 * i + 8, :] * avg[8 * i:8 * i + 8, :]
                sq[...] = sq[...] + part
                if mat == 1:
                    @pl.when(k >= CHUNKS - early)
                    def _():
                        ag_copy(0, k - (CHUNKS - early), True).start()

        chained = (s % 2 == 0) | (s == STAGES - 1)
        first = jnp.where(chained, 26 + 6 * s + s // 4 - 2 * (s // 7), 2 * CHUNKS)
        second = jnp.where(chained, first + 3, 2 * CHUNKS)
        ag_range(early, first)

        fills = [whole(0, m1, own1, 2), whole(0, v1, sq_o, 3), whole(1, m2, own2, 2)]
        for copy in fills:
            copy.start()
        for k in range(SLOTS):
            load_rows(0, k, w1.at[0]).start()
            load_rows(1, k, w2.at[0]).start()
            load_v2(k, v2.at[0]).start()

        partial = jnp.sum(sq1[...], keepdims=True) + jnp.sum(sq2[...], keepdims=True)
        nbuf[pair] = jnp.broadcast_to(partial, (8, 128))
        norm_copies = []
        for q in range(1, REPLICAS):
            other = (pair + q) % REPLICAS
            norm_copies.append(remote(nbuf.at[pair], nbuf.at[pair], n_snd.at[q], n_rcv.at[pair], r, 2 * other + (other + plane) % 2))
            norm_copies[-1].start()
        for q in range(1, REPLICAS):
            other = (pair + q) % REPLICAS
            arrive(nbuf.at[other], n_rcv.at[other])
        nplane[plane] = (nbuf[0] + nbuf[1]) + (nbuf[2] + nbuf[3])
        norm_copies.append(remote(nplane.at[plane], nplane.at[plane], np_snd.at[0], np_rcv.at[0], r, partner))
        norm_copies[-1].start()
        arrive(nplane.at[1 - plane], np_rcv.at[1])
        norm_copies.append(remote(nplane.at[1 - plane], nplane.at[1 - plane], np_snd.at[1], np_rcv.at[2], r, partner))
        norm_copies[-1].start()
        total = nplane[0] + nplane[1]

        clip = clip_of(total, maxn[...])[0:1, 0:1]
        for copy in fills:
            copy.wait()

        @pl.loop(0, CHUNKS)
        def _(k):
            load_rows(0, k, w1.at[0]).wait()
            rows = ds(k, R1)
            moment, sq_moment = moments(own1[rows, :], sq_o[rows, :], clip * recv1[rows, :])
            b1[rows, :] = new_weight(ring1[k % SLOTS], moment, sq_moment).astype(BF16)
            own1[rows, :] = moment
            sq_o[rows, :] = sq_moment

            @pl.when(k + SLOTS < CHUNKS)
            def _():
                load_rows(0, k + SLOTS, w1.at[0]).start()

        @pl.loop(0, CHUNKS)
        def _(k):
            load_rows(1, k, w2.at[0]).wait()
            load_v2(k, v2.at[0]).wait()
            rows = ds(k, R2)
            moment, sq_moment = moments(own2[rows, :], ringv[k % SLOTS], clip * recv2[rows, :])
            b2[rows, :] = new_weight(ring2[k % SLOTS], moment, sq_moment).astype(BF16)
            own2[rows, :] = moment
            ringv[k % SLOTS] = sq_moment
            store_v2(k).start()

            @pl.when(k + SLOTS < CHUNKS)
            def _():
                load_rows(1, k + SLOTS, w2.at[0]).start()

            @pl.when((k >= SLOTS // 2) & (k + SLOTS // 2 < CHUNKS))
            def _():
                store_v2(k - SLOTS // 2).wait()
                load_v2(k + SLOTS // 2, v2.at[0]).start()

        each((1,), lambda mat, k: store_v2(k).wait(), CHUNKS - SLOTS, CHUNKS)

        @pl.when(s == 0)
        def _():
            gathered(xbuf, in_rcv)

        @pl.when(s != 0)
        def _():
            arrive(xbuf, x_rcv)

        ag_range(first, second)

        @pl.loop(0, FF // TILE)
        def _(j):
            cols = ds(j, TILE)
            hid[:, cols] = gelu(mm(xbuf[...], b1[:, cols], NN)).astype(BF16)

        @pl.loop(0, D // TILE)
        def _(j):
            ybuf[:, ds(j, TILE)] = mm(hid[...], b2[:, ds(j, TILE)], NN).astype(BF16)

        send_x = remote(ybuf, xbuf, x_snd, x_rcv, owner_of(s + 1), (s + 1) % STAGES)

        @pl.when(s != STAGES - 1)
        def _():
            send_x.start()

        y_rows = ybuf.at[ds(r, TOK), :]

        @pl.when(s == STAGES - 1)
        def _():
            keep = pltpu.make_async_copy(y_rows, y_o, loc.at[2])
            keep.start()
            for q in range(1, REPLICAS):
                remote(ybuf.at[ds(own_r + q * away, TOK), :], y_o, y_snd.at[q + STAGES], y_rcv, own_r + q * away, s).start()
            keep.wait()
            for t in range(1, STAGES):
                remote(y_o, y_o, y_snd.at[t], y_rcv, r, (s + t) % STAGES).start()

        ag_range(second, 2 * CHUNKS)

        @pl.when(s == STAGES - 1)
        def _():
            for q in range(1, REPLICAS):
                remote(ybuf.at[ds(own_r + q * away, TOK), :], y_o, y_snd.at[q + STAGES], y_rcv, own_r + q * away, s).wait_send()

        @pl.when(s != 0)
        def _():
            send_g.wait_send()

        @pl.when(s != STAGES - 1)
        def _():
            send_x.wait_send()

        for copy in norm_copies:
            copy.wait_send()

        for k in range(SLOTS):
            load_rows(0, k, w1.at[0]).start()
            load_rows(1, k, w2.at[0]).start()
            load_v2(k, v2_o).start()

        @pl.loop(0, CHUNKS)
        def _(k):
            ag_copy(0, k, True).wait_send()
            load_rows(0, k, w1.at[0]).wait()
            rows = ds(k, R1)
            recv1[rows, :] = new_weight(ring1[k % SLOTS], own1[rows, :], sq_o[rows, :])

            @pl.when(k + SLOTS < CHUNKS)
            def _():
                load_rows(0, k + SLOTS, w1.at[0]).start()

        @pl.loop(0, CHUNKS)
        def _(k):
            ag_copy(1, k, True).wait_send()
            load_rows(1, k, w2.at[0]).wait()
            load_v2(k, v2_o).wait()
            rows = ds(k, R2)
            recv2[rows, :] = new_weight(ring2[k % SLOTS], own2[rows, :], ringv[k % SLOTS])

            @pl.when(k + SLOTS < CHUNKS)
            def _():
                load_rows(1, k + SLOTS, w2.at[0]).start()
                load_v2(k + SLOTS, v2_o).start()

    @pl.when(s != STAGES - 1)
    def _():
        arrive(y_o, y_rcv)

    @pl.when(s == STAGES - 1)
    def _():
        for t in range(1, STAGES):
            remote(y_o, y_o, y_snd.at[t], y_rcv, r, (s + t) % STAGES).wait_send()


def flush_kernel(*refs):
    source, target, (buf, rsem, wsem) = refs[5], refs[11], refs[12:]
    keep = pltpu.make_async_copy(refs[4], refs[10], wsem.at[FLUSH])
    keep.start()
    height = FF // FLUSH

    def copies(k):
        rows = pl.ds(k * height, height)
        return (pltpu.make_async_copy(source.at[rows, :], buf.at[rows, :], rsem.at[k]),
                pltpu.make_async_copy(buf.at[rows, :], target.at[rows, :], wsem.at[k]))

    for k in range(FLUSH):
        copies(k)[0].start()
    for k in range(FLUSH):
        copies(k)[0].wait()
        copies(k)[1].start()
    for k in range(FLUSH):
        copies(k)[1].wait()
    keep.wait()


def solution(mesh):
    assert mesh.shape["stage"] == STAGES and mesh.shape["data"] == REPLICAS
    weight_spec = P("stage", None, None)
    acc_spec = P("data", "stage", None, None)

    def local_step(w_in, w_out, mom_in, mom_out, sq_in, sq_out, acc_in, acc_out, stage_acts, grad_y, x_next, max_norm):
        maxn = jnp.full((8, 128), max_norm, F32)
        hbm = pl.BlockSpec(memory_space=pl.ANY)
        vmem = pl.BlockSpec(memory_space=pltpu.VMEM)
        dma = pltpu.SemaphoreType.DMA
        wide, tall = pltpu.VMEM((D, FF), F32), pltpu.VMEM((FF, D), F32)
        *kept, sq_out_new, _, _, y_next = pl.pallas_call(
            step_kernel,
            out_shape=(
                wide, tall, wide, tall, wide,
                jax.ShapeDtypeStruct((FF, D), F32), jax.ShapeDtypeStruct((D, FF), F32), jax.ShapeDtypeStruct((FF, D), F32),
                jax.ShapeDtypeStruct((TOK, D), BF16),
            ),
            in_specs=[hbm] * 11 + [vmem],
            out_specs=(vmem,) * 5 + (hbm,) * 4,
            scratch_shapes=[
                pltpu.VMEM((D, FF), BF16), pltpu.VMEM((FF, D), BF16), pltpu.VMEM((ROWS, FF), BF16),
                pltpu.VMEM((SLOTS, R1, FF), F32), pltpu.VMEM((SLOTS, R2, D), F32), pltpu.VMEM((SLOTS, R2, D), F32),
                pltpu.VMEM((ROWS, D), BF16), pltpu.VMEM((ROWS, D), BF16), pltpu.VMEM((ROWS, D), BF16),
                pltpu.VMEM((ROWS, D), BF16), pltpu.VMEM((ROWS, D), BF16),
                pltpu.VMEM((8, FF), F32), pltpu.VMEM((8, D), F32),
                pltpu.VMEM((REPLICAS, 8, 128), F32), pltpu.VMEM((2, 8, 128), F32),
                dma, dma((REPLICAS,)), dma, dma((REPLICAS,)), dma, dma, dma, dma, dma((STAGES + REPLICAS,)), dma,
                dma((2 * CHUNKS,)), dma((2 * CHUNKS,)), dma((2 * CHUNKS,)), dma((2 * CHUNKS,)),
                dma((REPLICAS,)), dma((REPLICAS,)), dma((2,)), dma((3,)), dma((REPLICAS,)), dma,
                dma((2, 4)), dma((3 * SLOTS,)), dma((SLOTS,)), dma((3,)),
            ],
            compiler_params=pltpu.CompilerParams(has_side_effects=True, collective_id=0, vmem_limit_bytes=VMEM_LIMIT),
            name="step",
        )(w_in, w_out, mom_in, mom_out, sq_in, sq_out, acc_in, acc_out, stage_acts[0], grad_y, x_next[0], maxn)
        wide, tall = jax.ShapeDtypeStruct((D, FF), F32), jax.ShapeDtypeStruct((FF, D), F32)
        new = pl.pallas_call(
            flush_kernel,
            out_shape=(wide, tall, wide, tall, wide, tall),
            in_specs=[hbm] * 4 + [vmem, hbm],
            out_specs=(hbm,) * 6,
            input_output_aliases={i: i for i in range(4)},
            scratch_shapes=[pltpu.VMEM((FF, D), F32), dma((FLUSH,)), dma((FLUSH + 1,))],
            compiler_params=pltpu.CompilerParams(vmem_limit_bytes=10000000),
            name="flush",
        )(*kept[:4], pltpu.with_memory_space_constraint(kept[4], pltpu.VMEM), sq_out_new)
        return *(array[None] for array in new), y_next[None]

    in_specs = (weight_spec,) * 6 + (acc_spec, acc_spec, P("stage", "data", None), P("data", None), P(None, "data", None), P())
    out_specs = (weight_spec,) * 6 + (P(None, "data", None),)
    return jax.shard_map(local_step, mesh=mesh, in_specs=in_specs, out_specs=out_specs, check_vma=False)
```

```python
import math

import jax
import jax.numpy as jnp
from jax import lax
from jax.experimental import pallas as pl
from jax.experimental.pallas import tpu as pltpu
from jax.sharding import PartitionSpec as P

BETA_ONE = 0.9
BETA_TWO = 0.95
ADAM_EPS = 1e-8
WEIGHT_DECAY = 0.1
LR_GAIN = 0.2
CLIP_EPS = 1e-6
STEP_COUNT = 20
MESH = pl.DeviceIdType.MESH
F32, BF16 = jnp.float32, jnp.bfloat16

D, FF, STAGES, REPLICAS, TOK = 768, 3072, 8, 4, 64
ROWS = REPLICAS * TOK
CHUNKS = 48
R1, R2 = D // CHUNKS, FF // CHUNKS
GROUP = 8
LAG = 16
TILE = 256
SLOTS = 8
EARLY = (8, 2)
VMEM_LIMIT = 19800000
FLUSH = 4
LEARN_RATE = LR_GAIN * D ** -0.5
GELU_K = math.sqrt(2.0 / math.pi)
NT = (((1,), (1,)), ((), ()))
TN = (((0,), (0,)), ((), ()))
NN = (((1,), (0,)), ((), ()))


def mm(lhs, rhs, dims):
    return lax.dot_general(lhs, rhs, dims, preferred_element_type=F32)


def gelu_parts(z):
    zz = z * z
    tanh = jnp.tanh(GELU_K * (z + 0.044715 * (zz * z)))
    cdf = 0.5 * (1.0 + tanh)
    slope = cdf + (0.5 * z) * (1.0 - tanh * tanh) * (GELU_K * (1.0 + (3 * 0.044715) * zz))
    return z * cdf, slope


def gelu(z):
    return z * (0.5 * (1.0 + jnp.tanh(GELU_K * (z + 0.044715 * (z * z * z)))))


def clip_of(sq_norm, max_norm):
    return jnp.minimum(1.0, max_norm / (jnp.sqrt(sq_norm) + CLIP_EPS))


def moments(moment, sq_moment, gradient):
    return BETA_ONE * moment + (1.0 - BETA_ONE) * gradient, BETA_TWO * sq_moment + (1.0 - BETA_TWO) * gradient * gradient


def new_weight(weight, moment_new, sq_new):
    step = (LEARN_RATE / (1.0 - BETA_ONE ** STEP_COUNT)) * moment_new
    v_hat = sq_new * (1.0 / (1.0 - BETA_TWO ** STEP_COUNT))
    return weight * (1.0 - LEARN_RATE * WEIGHT_DECAY) - step / (jnp.sqrt(v_hat) + ADAM_EPS)


def owner_of(stage):
    return 3 * ((stage % 2 + (stage // 2) % 2) % 2)


def ds(index, size):
    return pl.ds(pl.multiple_of(index * size, size), size)


def step_kernel(w1, w2, m1, m2, v1, v2, acc1, acc2, a_in, gy_in, x_in, maxn,
                recv2, own2, first_o, v2_o, g1_o, g2_o, y_o,
                b1, b2, hid, ring1, ring2, ringv, abuf, gbuf, gnext, xbuf, ybuf, sq1, sq2, nbuf, nplane,
                a_snd, a_rcv, in_snd, in_rcv, g_snd, g_rcv, x_snd, x_rcv, y_snd, y_rcv, rs_snd, ag_snd, line_rcv,
                n_snd, n_rcv, np_snd, np_rcv, nt_snd, nt_rcv, ld, st, vo, loc):
    r = lax.axis_index("data")
    s = lax.axis_index("stage")
    own_r = owner_of(s)
    away = 1 - 2 * (own_r // 3)
    d = (r - own_r) * away
    partner = s + 1 - 2 * (s % 2)
    pair, plane = s // 2, r // 3
    early = EARLY[0] + (EARLY[1] - EARLY[0]) * (s % 2)
    recv1, own1, sq_o = (first_o.at[i] for i in range(3))
    accs, recvs, owns, gouts = (acc1, acc2), (recv1, recv2), (own1, own2), (g1_o, g2_o)
    rings, weights_hbm, moments_hbm = (ring1, ring2), (w1, w2), (m1, m2)
    heights = (R1, R2)
    gp, dz = first_o.at[2, pl.ds(0, ROWS), :], first_o.at[2, pl.ds(ROWS, ROWS), :]

    def remote(src, dst, snd, rcv, to_r, to_s):
        return pltpu.make_async_remote_copy(src_ref=src, dst_ref=dst, send_sem=snd, recv_sem=rcv,
                                            device_id=(to_r, to_s), device_id_type=MESH)

    def arrive(ref, sem):
        pltpu.make_async_copy(ref, ref, sem).wait()

    def gather(src, dst, snd, rcv):
        part = dst.at[ds(r, TOK), :]

        @pl.when(d == 0)
        def _():
            pltpu.make_async_copy(src, part, rcv.at[r]).start()

        @pl.when(d != 0)
        def _():
            remote(src, part, snd, rcv.at[r], own_r, s).start()

    def gathered(dst, rcv):
        for q in range(REPLICAS):
            arrive(dst.at[pl.ds(q * TOK, TOK), :], rcv.at[q])

    barrier = pltpu.get_barrier_semaphore()
    for q in range(1, REPLICAS):
        pl.semaphore_signal(barrier, inc=1, device_id=((r + q) % REPLICAS, s), device_id_type=MESH)

    @pl.when(d == 0)
    def _():
        for t in range(1, STAGES):
            peer = (s + t) % STAGES
            pl.semaphore_signal(barrier, inc=1, device_id=(owner_of(peer), peer), device_id_type=MESH)

    @pl.when(s != STAGES - 1)
    def _():
        pl.semaphore_signal(barrier, inc=1, device_id=(r, STAGES - 1), device_id_type=MESH)

    at_end = (r == 0) | (r == REPLICAS - 1)

    @pl.when(at_end)
    def _():
        pl.semaphore_signal(barrier, inc=1, device_id=(r, partner), device_id_type=MESH)

    signals = REPLICAS - 1 + jnp.where(at_end, 1, 0) + jnp.where(d == 0, STAGES - 1, 0) + jnp.where(s == STAGES - 1, STAGES - 1, 0)
    pl.semaphore_wait(barrier, signals)

    @pl.when(s == STAGES - 1)
    def _():
        gather(gy_in, gbuf, in_snd, in_rcv)

    gather(a_in, abuf, a_snd, a_rcv)

    @pl.when(s == 0)
    def _():
        gather(x_in, xbuf, in_snd, in_rcv)

    def rs_copy(mat, k, src):
        part = recvs[mat].at[ds(k, heights[mat]), :]
        sem = mat * CHUNKS + k
        return remote(src, part, rs_snd.at[mat], line_rcv.at[sem], r - away, s)

    def rs_src(mat, k):
        return owns[mat].at[ds(k, heights[mat]), :]

    def ag_copy(mat, k, from_vmem):
        rows = ds(k, heights[mat])
        src = recvs[mat] if from_vmem else gouts[mat]
        sem = mat * CHUNKS + k
        return remote(src.at[rows, :], gouts[mat].at[rows, :], ag_snd.at[sem // GROUP], line_rcv.at[sem], r + away, s)

    def sent(mat, group):
        arrive(gouts[mat].at[ds(group, GROUP * heights[mat]), :], ag_snd.at[mat * (CHUNKS // GROUP) + group])

    def ag_range(lo, hi):
        for mat in (0, 1):
            @pl.loop(jnp.clip(lo - mat * CHUNKS, 0, CHUNKS), jnp.clip(hi - mat * CHUNKS, 0, CHUNKS))
            def _(k):
                ag_copy(mat, k, True).start()

    def each(mats, fn, lo=0, hi=CHUNKS):
        for mat in mats:
            @pl.loop(lo, hi)
            def _(k):
                fn(mat, k)

    @pl.when(d == 3)
    def _():
        parts = 4
        loads = [pltpu.make_async_copy(acc1.at[0, 0, pl.ds(q * D // parts, D // parts), :], own1.at[pl.ds(q * D // parts, D // parts), :], ld.at[0, q])
                 for q in range(parts)]
        loads.append(pltpu.make_async_copy(acc2.at[0, 0], own2, ld.at[1, 0]))
        for copy in loads:
            copy.start()
        for q in range(parts):
            loads[q].wait()
            each((0,), lambda mat, k: rs_copy(mat, k, rs_src(mat, k)).start(), q * CHUNKS // parts, (q + 1) * CHUNKS // parts)
        loads[parts].wait()
        each((1,), lambda mat, k: rs_copy(mat, k, rs_src(mat, k)).start())

    @pl.when((d == 1) | (d == 2))
    def _():
        own_copies = [pltpu.make_async_copy(accs[mat].at[0, 0], owns[mat], ld.at[mat, 0]) for mat in (0, 1)]
        for copy in own_copies:
            copy.start()
        for mat in (0, 1):
            own_copies[mat].wait()

            @pl.loop(0, CHUNKS)
            def _(k):
                rows = ds(k, heights[mat])
                arrive(recvs[mat].at[rows, :], line_rcv.at[mat * CHUNKS + k])
                recvs[mat][rows, :] = recvs[mat][rows, :] + owns[mat][rows, :]
                rs_copy(mat, k, recvs[mat].at[rows, :]).start()

    def load(mat, k, src, ring, sem):
        slot = k % SLOTS
        return pltpu.make_async_copy(src, ring.at[slot], st.at[sem * SLOTS + slot])

    def load_rows(mat, k, hbm):
        return load(mat, k, hbm.at[ds(k, heights[mat]), :], rings[mat], mat)

    def load_v2(k, hbm):
        return load(1, k, hbm.at[ds(k, R2), :], ringv, 2)

    def store_v2(k):
        return pltpu.make_async_copy(ringv.at[k % SLOTS], v2_o.at[ds(k, R2), :], vo.at[k % SLOTS])

    def whole(mat, src, dst, sem):
        return pltpu.make_async_copy(src.at[0], dst, ld.at[mat, sem])

    @pl.when(d != 0)
    def _():
        fills = ([whole(0, w1, recv1, 0), whole(0, m1, own1, 1), whole(0, v1, sq_o, 2)], [whole(1, w2, recv2, 0), whole(1, m2, own2, 1)])

        def prefetch():
            for mat in (0, 1):
                arrive(recvs[mat], rs_snd.at[mat])
            for copy in fills[0] + fills[1]:
                copy.start()

        def pass_on(mat, k):
            rows = ds(k, heights[mat])
            arrive(gouts[mat].at[rows, :], line_rcv.at[mat * CHUNKS + k])

            @pl.when(d != 3)
            def _():
                ag_copy(mat, k, False).start()

        @pl.when(d == 3)
        def _():
            prefetch()
            arrive(nplane.at[plane], np_rcv.at[0])
            remote(nplane.at[plane], nplane.at[plane], np_snd.at[0], np_rcv.at[1], own_r, s).start()
            arrive(nplane.at[1 - plane], np_rcv.at[2])
            for q in (1, 2):
                remote(nplane, nplane, nt_snd.at[q], nt_rcv, own_r + q * away, s).start()

        each((0,), pass_on, 0, LAG // 2)

        @pl.when(d != 3)
        def _():
            prefetch()

        each((0,), pass_on, LAG // 2, LAG)

        @pl.when(d != 3)
        def _():
            arrive(nplane, nt_rcv)

        clip = clip_of(nplane[0] + nplane[1], maxn[0, 0])[0:1, 0:1]
        for copy in fills[0]:
            copy.wait()

        def update_first(k):
            load_rows(0, k, g1_o).wait()
            rows = ds(k, R1)
            moment, sq_moment = moments(own1[rows, :], sq_o[rows, :], clip * ring1[k % SLOTS])
            recv1[rows, :] = new_weight(recv1[rows, :], moment, sq_moment)
            own1[rows, :] = moment
            sq_o[rows, :] = sq_moment

        def update_second(k):
            load_rows(1, k, g2_o).wait()
            load_v2(k, v2.at[0]).wait()
            rows = ds(k, R2)
            moment, sq_moment = moments(own2[rows, :], ringv[k % SLOTS], clip * ring2[k % SLOTS])
            recv2[rows, :] = new_weight(recv2[rows, :], moment, sq_moment)
            own2[rows, :] = moment
            ringv[k % SLOTS] = sq_moment
            store_v2(k).start()

        @pl.loop(LAG, 2 * LAG)
        def _(k):
            pass_on(0, k)
            for i in (0, 1):
                load_rows(0, 2 * (k - LAG) + i, g1_o).start()

            @pl.when(k > LAG)
            def _():
                for i in (0, 1):
                    update_first(2 * (k - LAG - 1) + i)

        update_first(2 * LAG - 2)

        @pl.loop(2 * LAG, CHUNKS)
        def _(k):
            pass_on(0, k)
            load_rows(0, k, g1_o).start()
            update_first(k - 1)

        update_first(CHUNKS - 1)
        for copy in fills[1]:
            copy.wait()

        @pl.loop(0, CHUNKS)
        def _(k):
            pass_on(1, k)

            @pl.when(k >= SLOTS)
            def _():
                store_v2(k - SLOTS).wait()

            load_rows(1, k, g2_o).start()
            load_v2(k, v2.at[0]).start()

            @pl.when(k > 0)
            def _():
                update_second(k - 1)

            @pl.when((s == STAGES - 1) & (k == CHUNKS - 8))
            def _():
                arrive(y_o, y_rcv)
                for t in range(1, STAGES):
                    remote(y_o, y_o, y_snd.at[t], y_rcv, r, (s + t) % STAGES).start()

        update_second(CHUNKS - 1)
        each((1,), lambda mat, k: store_v2(k).wait(), CHUNKS - SLOTS, CHUNKS)

        @pl.when(d == 3)
        def _():
            remote(nplane.at[plane], nplane.at[plane], np_snd.at[0], np_rcv.at[1], own_r, s).wait_send()
            for q in (1, 2):
                remote(nplane, nplane, nt_snd.at[q], nt_rcv, own_r + q * away, s).wait_send()

        remote(a_in, abuf.at[ds(r, TOK), :], a_snd, a_rcv.at[r], own_r, s).wait_send()

        @pl.when((s == 0) | (s == STAGES - 1))
        def _():
            remote(x_in, xbuf.at[ds(r, TOK), :], in_snd, in_rcv.at[r], own_r, s).wait_send()

        @pl.when(d != 3)
        def _():
            each((0, 1), sent, 0, CHUNKS // GROUP)

    @pl.when(d == 0)
    def _():
        loads = [pltpu.make_async_copy(w.at[0], own, ld.at[mat, 0]) for mat, (w, own) in enumerate(((w1, own1), (w2, own2)))]
        for copy in loads:
            copy.start()
        sq1[...] = jnp.zeros_like(sq1)
        sq2[...] = jnp.zeros_like(sq2)
        loads[0].wait()

        @pl.loop(0, CHUNKS)
        def _(k):
            b1[ds(k, R1), :] = own1[ds(k, R1), :].astype(BF16)

        loads[1].wait()

        @pl.loop(0, CHUNKS)
        def _(k):
            b2[ds(k, R2), :] = own2[ds(k, R2), :].astype(BF16)

        own_copies = [pltpu.make_async_copy(accs[mat].at[0, 0], owns[mat], ld.at[mat, 1]) for mat in (0, 1)]
        for copy in own_copies:
            copy.start()

        gathered(abuf, a_rcv)

        @pl.loop(0, FF // TILE)
        def _(j):
            cols = ds(j, TILE)
            value, slope = gelu_parts(mm(abuf[...], b1[:, cols], NN))
            hid[:, cols] = value.astype(BF16)
            gp[:, cols] = slope

        @pl.when(s == STAGES - 1)
        def _():
            gathered(gbuf, in_rcv)

        @pl.when(s != STAGES - 1)
        def _():
            arrive(gbuf, g_rcv)

        @pl.loop(0, FF // TILE)
        def _(j):
            cols = ds(j, TILE)
            dz[:, cols] = (gp[:, cols] * mm(gbuf[...], b2[cols, :], NT)).astype(BF16).astype(F32)

        send_g = remote(gnext, gbuf, g_snd, g_rcv, owner_of(s + STAGES - 1), (s + STAGES - 1) % STAGES)

        @pl.when(s != 0)
        def _():
            @pl.loop(0, D // TILE)
            def _(j):
                gnext[:, ds(j, TILE)] = mm(dz[...].astype(BF16), b1[ds(j, TILE), :], NT).astype(BF16)

            send_g.start()

        own_copies[0].wait()

        @pl.loop(0, FF // TILE)
        def _(j):
            cols = ds(j, TILE)
            own1[:, cols] = own1[:, cols] + mm(abuf[...], dz[:, cols].astype(BF16), TN)

        own_copies[1].wait()

        @pl.loop(0, FF // TILE)
        def _(j):
            cols = ds(j, TILE)
            own2[cols, :] = own2[cols, :] + mm(hid[:, cols], gbuf[...], TN)

        for mat in (0, 1):
            sq = (sq1, sq2)[mat]

            @pl.loop(0, CHUNKS)
            def _(k):
                rows = ds(k, heights[mat])
                arrive(recvs[mat].at[rows, :], line_rcv.at[mat * CHUNKS + k])
                avg = (recvs[mat][rows, :] + owns[mat][rows, :]) * (1.0 / REPLICAS)
                recvs[mat][rows, :] = avg
                part = avg[0:8, :] * avg[0:8, :]
                for i in range(1, heights[mat] // 8):
                    part = part + avg[8 * i:8 * i + 8, :] * avg[8 * i:8 * i + 8, :]
                sq[...] = sq[...] + part
                if mat == 1:
                    @pl.when(k >= CHUNKS - early)
                    def _():
                        ag_copy(0, k - (CHUNKS - early), True).start()

        chained = (s % 2 == 0) | (s == STAGES - 1)
        first = jnp.where(chained, 26 + 6 * s + s // 4 - 2 * (s // 7), 2 * CHUNKS)
        second = jnp.where(chained, first + 3, 2 * CHUNKS)
        ag_range(early, first)

        fills = [whole(0, m1, own1, 2), whole(0, v1, sq_o, 3), whole(1, m2, own2, 2)]
        for copy in fills:
            copy.start()
        for k in range(SLOTS):
            load_rows(0, k, w1.at[0]).start()
            load_rows(1, k, w2.at[0]).start()
            load_v2(k, v2.at[0]).start()

        partial = jnp.sum(sq1[...], keepdims=True) + jnp.sum(sq2[...], keepdims=True)
        nbuf[pair] = jnp.broadcast_to(partial, (8, 128))
        norm_copies = []
        for q in range(1, REPLICAS):
            other = (pair + q) % REPLICAS
            norm_copies.append(remote(nbuf.at[pair], nbuf.at[pair], n_snd.at[q], n_rcv.at[pair], r, 2 * other + (other + plane) % 2))
            norm_copies[-1].start()
        for q in range(1, REPLICAS):
            other = (pair + q) % REPLICAS
            arrive(nbuf.at[other], n_rcv.at[other])
        nplane[plane] = (nbuf[0] + nbuf[1]) + (nbuf[2] + nbuf[3])
        norm_copies.append(remote(nplane.at[plane], nplane.at[plane], np_snd.at[0], np_rcv.at[0], r, partner))
        norm_copies[-1].start()
        arrive(nplane.at[1 - plane], np_rcv.at[1])
        norm_copies.append(remote(nplane.at[1 - plane], nplane.at[1 - plane], np_snd.at[1], np_rcv.at[2], r, partner))
        norm_copies[-1].start()
        total = nplane[0] + nplane[1]

        clip = clip_of(total, maxn[0, 0])[0:1, 0:1]
        for copy in fills:
            copy.wait()

        @pl.loop(0, CHUNKS)
        def _(k):
            load_rows(0, k, w1.at[0]).wait()
            rows = ds(k, R1)
            moment, sq_moment = moments(own1[rows, :], sq_o[rows, :], clip * recv1[rows, :])
            b1[rows, :] = new_weight(ring1[k % SLOTS], moment, sq_moment).astype(BF16)
            own1[rows, :] = moment
            sq_o[rows, :] = sq_moment

            @pl.when(k + SLOTS < CHUNKS)
            def _():
                load_rows(0, k + SLOTS, w1.at[0]).start()

        @pl.loop(0, CHUNKS)
        def _(k):
            load_rows(1, k, w2.at[0]).wait()
            load_v2(k, v2.at[0]).wait()
            rows = ds(k, R2)
            moment, sq_moment = moments(own2[rows, :], ringv[k % SLOTS], clip * recv2[rows, :])
            b2[rows, :] = new_weight(ring2[k % SLOTS], moment, sq_moment).astype(BF16)
            own2[rows, :] = moment
            ringv[k % SLOTS] = sq_moment
            store_v2(k).start()

            @pl.when(k + SLOTS < CHUNKS)
            def _():
                load_rows(1, k + SLOTS, w2.at[0]).start()

            @pl.when((k >= SLOTS // 2) & (k + SLOTS // 2 < CHUNKS))
            def _():
                store_v2(k - SLOTS // 2).wait()
                load_v2(k + SLOTS // 2, v2.at[0]).start()

        each((1,), lambda mat, k: store_v2(k).wait(), CHUNKS - SLOTS, CHUNKS)

        @pl.when(s == 0)
        def _():
            gathered(xbuf, in_rcv)

        @pl.when(s != 0)
        def _():
            arrive(xbuf, x_rcv)

        ag_range(first, second)

        @pl.loop(0, FF // TILE)
        def _(j):
            cols = ds(j, TILE)
            hid[:, cols] = gelu(mm(xbuf[...], b1[:, cols], NN)).astype(BF16)

        @pl.loop(0, D // TILE)
        def _(j):
            ybuf[:, ds(j, TILE)] = mm(hid[...], b2[:, ds(j, TILE)], NN).astype(BF16)

        send_x = remote(ybuf, xbuf, x_snd, x_rcv, owner_of(s + 1), (s + 1) % STAGES)

        @pl.when(s != STAGES - 1)
        def _():
            send_x.start()

        y_rows = ybuf.at[ds(r, TOK), :]

        @pl.when(s == STAGES - 1)
        def _():
            keep = pltpu.make_async_copy(y_rows, y_o, loc.at[2])
            keep.start()
            for q in range(1, REPLICAS):
                remote(ybuf.at[ds(own_r + q * away, TOK), :], y_o, y_snd.at[q + STAGES], y_rcv, own_r + q * away, s).start()
            keep.wait()
            for t in range(1, STAGES):
                remote(y_o, y_o, y_snd.at[t], y_rcv, r, (s + t) % STAGES).start()

        ag_range(second, 2 * CHUNKS)

        @pl.when(s == STAGES - 1)
        def _():
            for q in range(1, REPLICAS):
                remote(ybuf.at[ds(own_r + q * away, TOK), :], y_o, y_snd.at[q + STAGES], y_rcv, own_r + q * away, s).wait_send()

        @pl.when(s != 0)
        def _():
            send_g.wait_send()

        @pl.when(s != STAGES - 1)
        def _():
            send_x.wait_send()

        for copy in norm_copies:
            copy.wait_send()

        for k in range(SLOTS):
            load_rows(0, k, w1.at[0]).start()
            load_rows(1, k, w2.at[0]).start()
            load_v2(k, v2_o).start()

        @pl.loop(0, CHUNKS)
        def _(k):
            @pl.when(k % GROUP == 0)
            def _():
                sent(0, k // GROUP)

            load_rows(0, k, w1.at[0]).wait()
            rows = ds(k, R1)
            recv1[rows, :] = new_weight(ring1[k % SLOTS], own1[rows, :], sq_o[rows, :])

            @pl.when(k + SLOTS < CHUNKS)
            def _():
                load_rows(0, k + SLOTS, w1.at[0]).start()

        @pl.loop(0, CHUNKS)
        def _(k):
            @pl.when(k % GROUP == 0)
            def _():
                sent(1, k // GROUP)

            load_rows(1, k, w2.at[0]).wait()
            load_v2(k, v2_o).wait()
            rows = ds(k, R2)
            recv2[rows, :] = new_weight(ring2[k % SLOTS], own2[rows, :], ringv[k % SLOTS])

            @pl.when(k + SLOTS < CHUNKS)
            def _():
                load_rows(1, k + SLOTS, w2.at[0]).start()
                load_v2(k + SLOTS, v2_o).start()

    @pl.when(s != STAGES - 1)
    def _():
        arrive(y_o, y_rcv)

    @pl.when(s == STAGES - 1)
    def _():
        for t in range(1, STAGES):
            remote(y_o, y_o, y_snd.at[t], y_rcv, r, (s + t) % STAGES).wait_send()


def flush_kernel(w_second, m_second, first, v_second, w_out, m_out, w_first, m_first, v_first, v_out, buf, rsem, wsem):
    height = FF // FLUSH

    def parts(k):
        rows = pl.ds(k * height, height)
        return (pltpu.make_async_copy(v_second.at[rows, :], buf.at[rows, :], rsem.at[k]),
                pltpu.make_async_copy(buf.at[rows, :], v_out.at[rows, :], wsem.at[k]))

    copies = [pltpu.make_async_copy(first.at[i], target, wsem.at[FLUSH + i]) for i, target in enumerate((w_first, m_first, v_first))]
    for k in range(FLUSH):
        parts(k)[0].start()
    for copy in copies:
        copy.start()
    for k in range(FLUSH):
        parts(k)[0].wait()
        parts(k)[1].start()
    for k in range(FLUSH):
        parts(k)[1].wait()
    for copy in copies:
        copy.wait()


def solution(mesh):
    assert mesh.shape["stage"] == STAGES and mesh.shape["data"] == REPLICAS
    weight_spec = P("stage", None, None)
    acc_spec = P("data", "stage", None, None)

    def local_step(w_in, w_out, mom_in, mom_out, sq_in, sq_out, acc_in, acc_out, stage_acts, grad_y, x_next, max_norm):
        maxn = max_norm.reshape(1, 1)
        hbm = pl.BlockSpec(memory_space=pl.ANY)
        vmem = pl.BlockSpec(memory_space=pltpu.VMEM)
        dma = pltpu.SemaphoreType.DMA
        tall = pltpu.VMEM((FF, D), F32)
        w_second, m_second, first, v_second, _, _, y_next = pl.pallas_call(
            step_kernel,
            out_shape=(
                tall, tall, pltpu.VMEM((3, D, FF), F32),
                jax.ShapeDtypeStruct((FF, D), F32), jax.ShapeDtypeStruct((D, FF), F32), jax.ShapeDtypeStruct((FF, D), F32),
                jax.ShapeDtypeStruct((TOK, D), BF16),
            ),
            in_specs=[hbm] * 11 + [pl.BlockSpec(memory_space=pltpu.SMEM)],
            out_specs=(vmem,) * 3 + (hbm,) * 4,
            scratch_shapes=[
                pltpu.VMEM((D, FF), BF16), pltpu.VMEM((FF, D), BF16), pltpu.VMEM((ROWS, FF), BF16),
                pltpu.VMEM((SLOTS, R1, FF), F32), pltpu.VMEM((SLOTS, R2, D), F32), pltpu.VMEM((SLOTS, R2, D), F32),
                pltpu.VMEM((ROWS, D), BF16), pltpu.VMEM((ROWS, D), BF16), pltpu.VMEM((ROWS, D), BF16),
                pltpu.VMEM((ROWS, D), BF16), pltpu.VMEM((ROWS, D), BF16),
                pltpu.VMEM((8, FF), F32), pltpu.VMEM((8, D), F32),
                pltpu.VMEM((REPLICAS, 8, 128), F32), pltpu.VMEM((2, 8, 128), F32),
                dma, dma((REPLICAS,)), dma, dma((REPLICAS,)), dma, dma, dma, dma, dma((STAGES + REPLICAS,)), dma,
                dma((2,)), dma((2 * CHUNKS // GROUP,)), dma((2 * CHUNKS,)),
                dma((REPLICAS,)), dma((REPLICAS,)), dma((2,)), dma((3,)), dma((REPLICAS,)), dma,
                dma((2, 4)), dma((3 * SLOTS,)), dma((SLOTS,)), dma((3,)),
            ],
            compiler_params=pltpu.CompilerParams(has_side_effects=True, collective_id=0, vmem_limit_bytes=VMEM_LIMIT),
            name="step",
        )(w_in, w_out, mom_in, mom_out, sq_in, sq_out, acc_in, acc_out, stage_acts[0], grad_y, x_next[0], maxn)
        wide, tall = jax.ShapeDtypeStruct((D, FF), F32), jax.ShapeDtypeStruct((FF, D), F32)
        w_out_new, m_out_new, w_in_new, m_in_new, v_in_new, v_out_new = pl.pallas_call(
            flush_kernel,
            out_shape=(tall, tall, wide, wide, wide, tall),
            in_specs=[hbm, hbm, vmem, hbm],
            out_specs=(hbm,) * 6,
            input_output_aliases={0: 0, 1: 1},
            scratch_shapes=[pltpu.VMEM((FF, D), F32), dma((FLUSH,)), dma((FLUSH + 3,))],
            compiler_params=pltpu.CompilerParams(vmem_limit_bytes=10000000),
            name="flush",
        )(w_second, m_second, pltpu.with_memory_space_constraint(first, pltpu.VMEM), v_second)
        new = (w_in_new, w_out_new, m_in_new, m_out_new, v_in_new, v_out_new)
        return *(array[None] for array in new), y_next[None]

    in_specs = (weight_spec,) * 6 + (acc_spec, acc_spec, P("stage", "data", None), P("data", None), P(None, "data", None), P())
    out_specs = (weight_spec,) * 6 + (P(None, "data", None),)
    return jax.shard_map(local_step, mesh=mesh, in_specs=in_specs, out_specs=out_specs, check_vma=False)
```

```python
import math

import jax
import jax.numpy as jnp
from jax import lax
from jax.experimental import pallas as pl
from jax.experimental.pallas import tpu as pltpu
from jax.sharding import PartitionSpec as P

BETA_ONE = 0.9
BETA_TWO = 0.95
ADAM_EPS = 1e-8
WEIGHT_DECAY = 0.1
LR_GAIN = 0.2
CLIP_EPS = 1e-6
STEP_COUNT = 20
MESH = pl.DeviceIdType.MESH
F32, BF16 = jnp.float32, jnp.bfloat16

D, FF, STAGES, REPLICAS, TOK = 768, 3072, 8, 4, 64
ROWS = REPLICAS * TOK
CHUNKS = 48
R1, R2 = D // CHUNKS, FF // CHUNKS
GROUP = 8
LAG = 16
TILE = 256
SLOTS = 8
EARLY = (9, 2)
HEAD = (3, 0)
VMEM_LIMIT = 19800000
FLUSH = 4
LEARN_RATE = LR_GAIN * D ** -0.5
GELU_K = math.sqrt(2.0 / math.pi)
NT = (((1,), (1,)), ((), ()))
TN = (((0,), (0,)), ((), ()))
NN = (((1,), (0,)), ((), ()))


def mm(lhs, rhs, dims):
    return lax.dot_general(lhs, rhs, dims, preferred_element_type=F32)


def gelu_parts(z):
    zz = z * z
    tanh = jnp.tanh(GELU_K * (z + 0.044715 * (zz * z)))
    cdf = 0.5 * (1.0 + tanh)
    slope = cdf + (0.5 * z) * (1.0 - tanh * tanh) * (GELU_K * (1.0 + (3 * 0.044715) * zz))
    return z * cdf, slope


def gelu(z):
    return z * (0.5 * (1.0 + jnp.tanh(GELU_K * (z + 0.044715 * (z * z * z)))))


def clip_of(sq_norm, max_norm):
    return jnp.minimum(1.0, max_norm / (jnp.sqrt(sq_norm) + CLIP_EPS))


def moments(moment, sq_moment, gradient):
    return BETA_ONE * moment + (1.0 - BETA_ONE) * gradient, BETA_TWO * sq_moment + (1.0 - BETA_TWO) * gradient * gradient


def new_weight(weight, moment_new, sq_new):
    step = (LEARN_RATE / (1.0 - BETA_ONE ** STEP_COUNT)) * moment_new
    v_hat = sq_new * (1.0 / (1.0 - BETA_TWO ** STEP_COUNT))
    return weight * (1.0 - LEARN_RATE * WEIGHT_DECAY) - step / (jnp.sqrt(v_hat) + ADAM_EPS)


def owner_of(stage):
    return 3 * ((stage % 2 + (stage // 2) % 2) % 2)


def ds(index, size):
    return pl.ds(pl.multiple_of(index * size, size), size)


def step_kernel(w1, w2, m1, m2, v1, v2, acc1, acc2, a_in, gy_in, x_in, maxn,
                recv2, own2, first_o, v2_o, g1_o, g2_o, y_o,
                b1, b2, hid, ring1, ring2, ringv, abuf, gbuf, gnext, xbuf, ybuf, sq1, sq2, nbuf, nplane,
                a_snd, a_rcv, in_snd, in_rcv, g_snd, g_rcv, x_snd, x_rcv, y_snd, y_rcv, rs_snd, ag_snd, line_rcv,
                n_snd, n_rcv, np_snd, np_rcv, nt_snd, nt_rcv, ld, st, vo, loc):
    r = lax.axis_index("data")
    s = lax.axis_index("stage")
    own_r = owner_of(s)
    away = 1 - 2 * (own_r // 3)
    d = (r - own_r) * away
    partner = s + 1 - 2 * (s % 2)
    pair, plane = s // 2, r // 3
    early = EARLY[0] + (EARLY[1] - EARLY[0]) * (s % 2)
    head = jnp.where(d == 1, HEAD[0] + (HEAD[1] - HEAD[0]) * (s % 2), 0)
    recv1, own1, sq_o = (first_o.at[i] for i in range(3))
    accs, recvs, owns, gouts = (acc1, acc2), (recv1, recv2), (own1, own2), (g1_o, g2_o)
    rings, weights_hbm, moments_hbm = (ring1, ring2), (w1, w2), (m1, m2)
    heights = (R1, R2)
    gp, dz = first_o.at[2, pl.ds(0, ROWS), :], first_o.at[2, pl.ds(ROWS, ROWS), :]

    def remote(src, dst, snd, rcv, to_r, to_s):
        return pltpu.make_async_remote_copy(src_ref=src, dst_ref=dst, send_sem=snd, recv_sem=rcv,
                                            device_id=(to_r, to_s), device_id_type=MESH)

    def arrive(ref, sem):
        pltpu.make_async_copy(ref, ref, sem).wait()

    def gather(src, dst, snd, rcv):
        part = dst.at[ds(r, TOK), :]

        @pl.when(d == 0)
        def _():
            pltpu.make_async_copy(src, part, rcv.at[r]).start()

        @pl.when(d != 0)
        def _():
            remote(src, part, snd, rcv.at[r], own_r, s).start()

    def gathered(dst, rcv):
        for q in range(REPLICAS):
            arrive(dst.at[pl.ds(q * TOK, TOK), :], rcv.at[q])

    barrier = pltpu.get_barrier_semaphore()
    for q in range(1, REPLICAS):
        pl.semaphore_signal(barrier, inc=1, device_id=((r + q) % REPLICAS, s), device_id_type=MESH)

    @pl.when(d == 0)
    def _():
        for t in range(1, STAGES):
            peer = (s + t) % STAGES
            pl.semaphore_signal(barrier, inc=1, device_id=(owner_of(peer), peer), device_id_type=MESH)

    @pl.when(s != STAGES - 1)
    def _():
        pl.semaphore_signal(barrier, inc=1, device_id=(r, STAGES - 1), device_id_type=MESH)

    at_end = (r == 0) | (r == REPLICAS - 1)

    @pl.when(at_end)
    def _():
        pl.semaphore_signal(barrier, inc=1, device_id=(r, partner), device_id_type=MESH)

    signals = REPLICAS - 1 + jnp.where(at_end, 1, 0) + jnp.where(d == 0, STAGES - 1, 0) + jnp.where(s == STAGES - 1, STAGES - 1, 0)
    pl.semaphore_wait(barrier, signals)

    @pl.when(s == STAGES - 1)
    def _():
        gather(gy_in, gbuf, in_snd, in_rcv)

    gather(a_in, abuf, a_snd, a_rcv)

    @pl.when(s == 0)
    def _():
        gather(x_in, xbuf, in_snd, in_rcv)

    def rs_copy(mat, k, src):
        part = recvs[mat].at[ds(k, heights[mat]), :]
        sem = mat * CHUNKS + k
        return remote(src, part, rs_snd.at[mat], line_rcv.at[sem], r - away, s)

    def rs_src(mat, k):
        return owns[mat].at[ds(k, heights[mat]), :]

    def ag_copy(mat, k, from_vmem):
        rows = ds(k, heights[mat])
        src = recvs[mat] if from_vmem else gouts[mat]
        sem = mat * CHUNKS + k
        return remote(src.at[rows, :], gouts[mat].at[rows, :], ag_snd.at[sem // GROUP], line_rcv.at[sem], r + away, s)

    def sent(mat, group):
        arrive(gouts[mat].at[ds(group, GROUP * heights[mat]), :], ag_snd.at[mat * (CHUNKS // GROUP) + group])

    def ag_range(lo, hi):
        for mat in (0, 1):
            @pl.loop(jnp.clip(lo - mat * CHUNKS, 0, CHUNKS), jnp.clip(hi - mat * CHUNKS, 0, CHUNKS))
            def _(k):
                ag_copy(mat, k, True).start()

    def each(mats, fn, lo=0, hi=CHUNKS):
        for mat in mats:
            @pl.loop(lo, hi)
            def _(k):
                fn(mat, k)

    def pass_on(mat, k):
        rows = ds(k, heights[mat])
        arrive(gouts[mat].at[rows, :], line_rcv.at[mat * CHUNKS + k])

        @pl.when(d != 3)
        def _():
            ag_copy(mat, k, False).start()

    @pl.when(d == 3)
    def _():
        parts = 4
        loads = [pltpu.make_async_copy(acc1.at[0, 0, pl.ds(q * D // parts, D // parts), :], own1.at[pl.ds(q * D // parts, D // parts), :], ld.at[0, q])
                 for q in range(parts)]
        loads.append(pltpu.make_async_copy(acc2.at[0, 0], own2, ld.at[1, 0]))
        for copy in loads:
            copy.start()
        for q in range(parts):
            loads[q].wait()
            each((0,), lambda mat, k: rs_copy(mat, k, rs_src(mat, k)).start(), q * CHUNKS // parts, (q + 1) * CHUNKS // parts)
        loads[parts].wait()
        each((1,), lambda mat, k: rs_copy(mat, k, rs_src(mat, k)).start())

    @pl.when((d == 1) | (d == 2))
    def _():
        own_copies = [pltpu.make_async_copy(accs[mat].at[0, 0], owns[mat], ld.at[mat, 0]) for mat in (0, 1)]
        for copy in own_copies:
            copy.start()
        for mat in (0, 1):
            own_copies[mat].wait()

            @pl.loop(0, CHUNKS)
            def _(k):
                rows = ds(k, heights[mat])
                arrive(recvs[mat].at[rows, :], line_rcv.at[mat * CHUNKS + k])
                recvs[mat][rows, :] = recvs[mat][rows, :] + owns[mat][rows, :]
                rs_copy(mat, k, recvs[mat].at[rows, :]).start()
                if mat == 1:
                    @pl.when(k >= CHUNKS - head)
                    def _():
                        pass_on(0, k - (CHUNKS - head))

    def load(mat, k, src, ring, sem):
        slot = k % SLOTS
        return pltpu.make_async_copy(src, ring.at[slot], st.at[sem * SLOTS + slot])

    def load_rows(mat, k, hbm):
        return load(mat, k, hbm.at[ds(k, heights[mat]), :], rings[mat], mat)

    def load_v2(k, hbm):
        return load(1, k, hbm.at[ds(k, R2), :], ringv, 2)

    def store_v2(k):
        return pltpu.make_async_copy(ringv.at[k % SLOTS], v2_o.at[ds(k, R2), :], vo.at[k % SLOTS])

    def whole(mat, src, dst, sem):
        return pltpu.make_async_copy(src.at[0], dst, ld.at[mat, sem])

    @pl.when(d != 0)
    def _():
        fills = ([whole(0, w1, recv1, 0), whole(0, m1, own1, 1), whole(0, v1, sq_o, 2)], [whole(1, w2, recv2, 0), whole(1, m2, own2, 1)])

        def prefetch():
            for mat in (0, 1):
                arrive(recvs[mat], rs_snd.at[mat])
            for copy in fills[0] + fills[1]:
                copy.start()

        @pl.when(d == 3)
        def _():
            prefetch()
            arrive(nplane.at[plane], np_rcv.at[0])
            remote(nplane.at[plane], nplane.at[plane], np_snd.at[0], np_rcv.at[1], own_r, s).start()
            arrive(nplane.at[1 - plane], np_rcv.at[2])
            for q in (1, 2):
                remote(nplane, nplane, nt_snd.at[q], nt_rcv, own_r + q * away, s).start()

        each((0,), pass_on, head, LAG // 2)

        @pl.when(d != 3)
        def _():
            prefetch()

        each((0,), pass_on, LAG // 2, LAG)

        @pl.when(d != 3)
        def _():
            arrive(nplane, nt_rcv)

        clip = clip_of(nplane[0] + nplane[1], maxn[0, 0])[0:1, 0:1]
        for copy in fills[0]:
            copy.wait()

        def update_first(k):
            load_rows(0, k, g1_o).wait()
            rows = ds(k, R1)
            moment, sq_moment = moments(own1[rows, :], sq_o[rows, :], clip * ring1[k % SLOTS])
            recv1[rows, :] = new_weight(recv1[rows, :], moment, sq_moment)
            own1[rows, :] = moment
            sq_o[rows, :] = sq_moment

        def update_second(k):
            load_rows(1, k, g2_o).wait()
            load_v2(k, v2.at[0]).wait()
            rows = ds(k, R2)
            moment, sq_moment = moments(own2[rows, :], ringv[k % SLOTS], clip * ring2[k % SLOTS])
            recv2[rows, :] = new_weight(recv2[rows, :], moment, sq_moment)
            own2[rows, :] = moment
            ringv[k % SLOTS] = sq_moment
            store_v2(k).start()

        @pl.loop(LAG, 2 * LAG)
        def _(k):
            pass_on(0, k)
            for i in (0, 1):
                load_rows(0, 2 * (k - LAG) + i, g1_o).start()

            @pl.when(k > LAG)
            def _():
                for i in (0, 1):
                    update_first(2 * (k - LAG - 1) + i)

        update_first(2 * LAG - 2)

        @pl.loop(2 * LAG, CHUNKS)
        def _(k):
            pass_on(0, k)
            load_rows(0, k, g1_o).start()
            update_first(k - 1)

        update_first(CHUNKS - 1)
        for copy in fills[1]:
            copy.wait()

        @pl.loop(0, CHUNKS)
        def _(k):
            pass_on(1, k)

            @pl.when(k >= SLOTS)
            def _():
                store_v2(k - SLOTS).wait()

            load_rows(1, k, g2_o).start()
            load_v2(k, v2.at[0]).start()

            @pl.when(k > 0)
            def _():
                update_second(k - 1)

            @pl.when((s == STAGES - 1) & (k == CHUNKS - 8))
            def _():
                arrive(y_o, y_rcv)
                for t in range(1, STAGES):
                    remote(y_o, y_o, y_snd.at[t], y_rcv, r, (s + t) % STAGES).start()

        update_second(CHUNKS - 1)
        each((1,), lambda mat, k: store_v2(k).wait(), CHUNKS - SLOTS, CHUNKS)

        @pl.when(d == 3)
        def _():
            remote(nplane.at[plane], nplane.at[plane], np_snd.at[0], np_rcv.at[1], own_r, s).wait_send()
            for q in (1, 2):
                remote(nplane, nplane, nt_snd.at[q], nt_rcv, own_r + q * away, s).wait_send()

        remote(a_in, abuf.at[ds(r, TOK), :], a_snd, a_rcv.at[r], own_r, s).wait_send()

        @pl.when((s == 0) | (s == STAGES - 1))
        def _():
            remote(x_in, xbuf.at[ds(r, TOK), :], in_snd, in_rcv.at[r], own_r, s).wait_send()

        @pl.when(d != 3)
        def _():
            each((0, 1), sent, 0, CHUNKS // GROUP)

    @pl.when(d == 0)
    def _():
        loads = [pltpu.make_async_copy(w.at[0], own, ld.at[mat, 0]) for mat, (w, own) in enumerate(((w1, own1), (w2, own2)))]
        for copy in loads:
            copy.start()
        sq1[...] = jnp.zeros_like(sq1)
        sq2[...] = jnp.zeros_like(sq2)
        loads[0].wait()

        @pl.loop(0, CHUNKS)
        def _(k):
            b1[ds(k, R1), :] = own1[ds(k, R1), :].astype(BF16)

        loads[1].wait()

        @pl.loop(0, CHUNKS)
        def _(k):
            b2[ds(k, R2), :] = own2[ds(k, R2), :].astype(BF16)

        own_copies = [pltpu.make_async_copy(accs[mat].at[0, 0], owns[mat], ld.at[mat, 1]) for mat in (0, 1)]
        for copy in own_copies:
            copy.start()

        gathered(abuf, a_rcv)

        @pl.loop(0, FF // TILE)
        def _(j):
            cols = ds(j, TILE)
            value, slope = gelu_parts(mm(abuf[...], b1[:, cols], NN))
            hid[:, cols] = value.astype(BF16)
            gp[:, cols] = slope

        @pl.when(s == STAGES - 1)
        def _():
            gathered(gbuf, in_rcv)

        @pl.when(s != STAGES - 1)
        def _():
            arrive(gbuf, g_rcv)

        @pl.loop(0, FF // TILE)
        def _(j):
            cols = ds(j, TILE)
            dz[:, cols] = (gp[:, cols] * mm(gbuf[...], b2[cols, :], NT)).astype(BF16).astype(F32)

        send_g = remote(gnext, gbuf, g_snd, g_rcv, owner_of(s + STAGES - 1), (s + STAGES - 1) % STAGES)

        @pl.when(s != 0)
        def _():
            @pl.loop(0, D // TILE)
            def _(j):
                gnext[:, ds(j, TILE)] = mm(dz[...].astype(BF16), b1[ds(j, TILE), :], NT).astype(BF16)

            send_g.start()

        own_copies[0].wait()

        @pl.loop(0, FF // TILE)
        def _(j):
            cols = ds(j, TILE)
            own1[:, cols] = own1[:, cols] + mm(abuf[...], dz[:, cols].astype(BF16), TN)

        own_copies[1].wait()

        @pl.loop(0, FF // TILE)
        def _(j):
            cols = ds(j, TILE)
            own2[cols, :] = own2[cols, :] + mm(hid[:, cols], gbuf[...], TN)

        for mat in (0, 1):
            sq = (sq1, sq2)[mat]

            @pl.loop(0, CHUNKS)
            def _(k):
                rows = ds(k, heights[mat])
                arrive(recvs[mat].at[rows, :], line_rcv.at[mat * CHUNKS + k])
                avg = (recvs[mat][rows, :] + owns[mat][rows, :]) * (1.0 / REPLICAS)
                recvs[mat][rows, :] = avg
                part = avg[0:8, :] * avg[0:8, :]
                for i in range(1, heights[mat] // 8):
                    part = part + avg[8 * i:8 * i + 8, :] * avg[8 * i:8 * i + 8, :]
                sq[...] = sq[...] + part
                if mat == 1:
                    @pl.when(k >= CHUNKS - early)
                    def _():
                        ag_copy(0, k - (CHUNKS - early), True).start()

        chained = (s % 2 == 0) | (s == STAGES - 1)
        first = jnp.where(chained, 26 + 6 * s + s // 4 - 2 * (s // 7), 2 * CHUNKS)
        second = jnp.where(chained, first + 3, 2 * CHUNKS)
        ag_range(early, first)

        fills = [whole(0, m1, own1, 2), whole(0, v1, sq_o, 3), whole(1, m2, own2, 2)]
        for copy in fills:
            copy.start()
        for k in range(SLOTS):
            load_rows(0, k, w1.at[0]).start()
            load_rows(1, k, w2.at[0]).start()
            load_v2(k, v2.at[0]).start()

        partial = jnp.sum(sq1[...], keepdims=True) + jnp.sum(sq2[...], keepdims=True)
        nbuf[pair] = jnp.broadcast_to(partial, (8, 128))
        norm_copies = []
        for q in range(1, REPLICAS):
            other = (pair + q) % REPLICAS
            norm_copies.append(remote(nbuf.at[pair], nbuf.at[pair], n_snd.at[q], n_rcv.at[pair], r, 2 * other + (other + plane) % 2))
            norm_copies[-1].start()
        for q in range(1, REPLICAS):
            other = (pair + q) % REPLICAS
            arrive(nbuf.at[other], n_rcv.at[other])
        nplane[plane] = (nbuf[0] + nbuf[1]) + (nbuf[2] + nbuf[3])
        norm_copies.append(remote(nplane.at[plane], nplane.at[plane], np_snd.at[0], np_rcv.at[0], r, partner))
        norm_copies[-1].start()
        arrive(nplane.at[1 - plane], np_rcv.at[1])
        norm_copies.append(remote(nplane.at[1 - plane], nplane.at[1 - plane], np_snd.at[1], np_rcv.at[2], r, partner))
        norm_copies[-1].start()
        total = nplane[0] + nplane[1]

        clip = clip_of(total, maxn[0, 0])[0:1, 0:1]
        for copy in fills:
            copy.wait()

        @pl.loop(0, CHUNKS)
        def _(k):
            load_rows(0, k, w1.at[0]).wait()
            rows = ds(k, R1)
            moment, sq_moment = moments(own1[rows, :], sq_o[rows, :], clip * recv1[rows, :])
            b1[rows, :] = new_weight(ring1[k % SLOTS], moment, sq_moment).astype(BF16)
            own1[rows, :] = moment
            sq_o[rows, :] = sq_moment

            @pl.when(k + SLOTS < CHUNKS)
            def _():
                load_rows(0, k + SLOTS, w1.at[0]).start()

        @pl.loop(0, CHUNKS)
        def _(k):
            load_rows(1, k, w2.at[0]).wait()
            load_v2(k, v2.at[0]).wait()
            rows = ds(k, R2)
            moment, sq_moment = moments(own2[rows, :], ringv[k % SLOTS], clip * recv2[rows, :])
            b2[rows, :] = new_weight(ring2[k % SLOTS], moment, sq_moment).astype(BF16)
            own2[rows, :] = moment
            ringv[k % SLOTS] = sq_moment
            store_v2(k).start()

            @pl.when(k + SLOTS < CHUNKS)
            def _():
                load_rows(1, k + SLOTS, w2.at[0]).start()

            @pl.when((k >= SLOTS // 2) & (k + SLOTS // 2 < CHUNKS))
            def _():
                store_v2(k - SLOTS // 2).wait()
                load_v2(k + SLOTS // 2, v2.at[0]).start()

        each((1,), lambda mat, k: store_v2(k).wait(), CHUNKS - SLOTS, CHUNKS)

        @pl.when(s == 0)
        def _():
            gathered(xbuf, in_rcv)

        @pl.when(s != 0)
        def _():
            arrive(xbuf, x_rcv)

        ag_range(first, second)

        @pl.loop(0, FF // TILE)
        def _(j):
            cols = ds(j, TILE)
            hid[:, cols] = gelu(mm(xbuf[...], b1[:, cols], NN)).astype(BF16)

        @pl.loop(0, D // TILE)
        def _(j):
            ybuf[:, ds(j, TILE)] = mm(hid[...], b2[:, ds(j, TILE)], NN).astype(BF16)

        send_x = remote(ybuf, xbuf, x_snd, x_rcv, owner_of(s + 1), (s + 1) % STAGES)

        @pl.when(s != STAGES - 1)
        def _():
            send_x.start()

        y_rows = ybuf.at[ds(r, TOK), :]

        @pl.when(s == STAGES - 1)
        def _():
            keep = pltpu.make_async_copy(y_rows, y_o, loc.at[2])
            keep.start()
            for q in range(1, REPLICAS):
                remote(ybuf.at[ds(own_r + q * away, TOK), :], y_o, y_snd.at[q + STAGES], y_rcv, own_r + q * away, s).start()
            keep.wait()
            for t in range(1, STAGES):
                remote(y_o, y_o, y_snd.at[t], y_rcv, r, (s + t) % STAGES).start()

        ag_range(second, 2 * CHUNKS)

        @pl.when(s == STAGES - 1)
        def _():
            for q in range(1, REPLICAS):
                remote(ybuf.at[ds(own_r + q * away, TOK), :], y_o, y_snd.at[q + STAGES], y_rcv, own_r + q * away, s).wait_send()

        @pl.when(s != 0)
        def _():
            send_g.wait_send()

        @pl.when(s != STAGES - 1)
        def _():
            send_x.wait_send()

        for copy in norm_copies:
            copy.wait_send()

        for k in range(SLOTS):
            load_rows(0, k, w1.at[0]).start()
            load_rows(1, k, w2.at[0]).start()
            load_v2(k, v2_o).start()

        @pl.loop(0, CHUNKS)
        def _(k):
            @pl.when(k % GROUP == 0)
            def _():
                sent(0, k // GROUP)

            load_rows(0, k, w1.at[0]).wait()
            rows = ds(k, R1)
            recv1[rows, :] = new_weight(ring1[k % SLOTS], own1[rows, :], sq_o[rows, :])

            @pl.when(k + SLOTS < CHUNKS)
            def _():
                load_rows(0, k + SLOTS, w1.at[0]).start()

        @pl.loop(0, CHUNKS)
        def _(k):
            @pl.when(k % GROUP == 0)
            def _():
                sent(1, k // GROUP)

            load_rows(1, k, w2.at[0]).wait()
            load_v2(k, v2_o).wait()
            rows = ds(k, R2)
            recv2[rows, :] = new_weight(ring2[k % SLOTS], own2[rows, :], ringv[k % SLOTS])

            @pl.when(k + SLOTS < CHUNKS)
            def _():
                load_rows(1, k + SLOTS, w2.at[0]).start()
                load_v2(k + SLOTS, v2_o).start()

    @pl.when(s != STAGES - 1)
    def _():
        arrive(y_o, y_rcv)

    @pl.when(s == STAGES - 1)
    def _():
        for t in range(1, STAGES):
            remote(y_o, y_o, y_snd.at[t], y_rcv, r, (s + t) % STAGES).wait_send()


def flush_kernel(w_second, m_second, first, v_second, w_out, m_out, w_first, m_first, v_first, v_out, buf, rsem, wsem):
    height = FF // FLUSH

    def parts(k):
        rows = pl.ds(k * height, height)
        return (pltpu.make_async_copy(v_second.at[rows, :], buf.at[rows, :], rsem.at[k]),
                pltpu.make_async_copy(buf.at[rows, :], v_out.at[rows, :], wsem.at[k]))

    copies = [pltpu.make_async_copy(first.at[i], target, wsem.at[FLUSH + i]) for i, target in enumerate((w_first, m_first, v_first))]
    for k in range(FLUSH):
        parts(k)[0].start()
    for copy in copies:
        copy.start()
    for k in range(FLUSH):
        parts(k)[0].wait()
        parts(k)[1].start()
    for k in range(FLUSH):
        parts(k)[1].wait()
    for copy in copies:
        copy.wait()


def solution(mesh):
    assert mesh.shape["stage"] == STAGES and mesh.shape["data"] == REPLICAS
    weight_spec = P("stage", None, None)
    acc_spec = P("data", "stage", None, None)

    def local_step(w_in, w_out, mom_in, mom_out, sq_in, sq_out, acc_in, acc_out, stage_acts, grad_y, x_next, max_norm):
        maxn = max_norm.reshape(1, 1)
        hbm = pl.BlockSpec(memory_space=pl.ANY)
        vmem = pl.BlockSpec(memory_space=pltpu.VMEM)
        dma = pltpu.SemaphoreType.DMA
        tall = pltpu.VMEM((FF, D), F32)
        w_second, m_second, first, v_second, _, _, y_next = pl.pallas_call(
            step_kernel,
            out_shape=(
                tall, tall, pltpu.VMEM((3, D, FF), F32),
                jax.ShapeDtypeStruct((FF, D), F32), jax.ShapeDtypeStruct((D, FF), F32), jax.ShapeDtypeStruct((FF, D), F32),
                jax.ShapeDtypeStruct((TOK, D), BF16),
            ),
            in_specs=[hbm] * 11 + [pl.BlockSpec(memory_space=pltpu.SMEM)],
            out_specs=(vmem,) * 3 + (hbm,) * 4,
            scratch_shapes=[
                pltpu.VMEM((D, FF), BF16), pltpu.VMEM((FF, D), BF16), pltpu.VMEM((ROWS, FF), BF16),
                pltpu.VMEM((SLOTS, R1, FF), F32), pltpu.VMEM((SLOTS, R2, D), F32), pltpu.VMEM((SLOTS, R2, D), F32),
                pltpu.VMEM((ROWS, D), BF16), pltpu.VMEM((ROWS, D), BF16), pltpu.VMEM((ROWS, D), BF16),
                pltpu.VMEM((ROWS, D), BF16), pltpu.VMEM((ROWS, D), BF16),
                pltpu.VMEM((8, FF), F32), pltpu.VMEM((8, D), F32),
                pltpu.VMEM((REPLICAS, 8, 128), F32), pltpu.VMEM((2, 8, 128), F32),
                dma, dma((REPLICAS,)), dma, dma((REPLICAS,)), dma, dma, dma, dma, dma((STAGES + REPLICAS,)), dma,
                dma((2,)), dma((2 * CHUNKS // GROUP,)), dma((2 * CHUNKS,)),
                dma((REPLICAS,)), dma((REPLICAS,)), dma((2,)), dma((3,)), dma((REPLICAS,)), dma,
                dma((2, 4)), dma((3 * SLOTS,)), dma((SLOTS,)), dma((3,)),
            ],
            compiler_params=pltpu.CompilerParams(has_side_effects=True, collective_id=0, vmem_limit_bytes=VMEM_LIMIT),
            name="step",
        )(w_in, w_out, mom_in, mom_out, sq_in, sq_out, acc_in, acc_out, stage_acts[0], grad_y, x_next[0], maxn)
        wide, tall = jax.ShapeDtypeStruct((D, FF), F32), jax.ShapeDtypeStruct((FF, D), F32)
        w_out_new, m_out_new, w_in_new, m_in_new, v_in_new, v_out_new = pl.pallas_call(
            flush_kernel,
            out_shape=(tall, tall, wide, wide, wide, tall),
            in_specs=[hbm, hbm, vmem, hbm],
            out_specs=(hbm,) * 6,
            input_output_aliases={0: 0, 1: 1},
            scratch_shapes=[pltpu.VMEM((FF, D), F32), dma((FLUSH,)), dma((FLUSH + 3,))],
            compiler_params=pltpu.CompilerParams(vmem_limit_bytes=10000000),
            name="flush",
        )(w_second, m_second, pltpu.with_memory_space_constraint(first, pltpu.VMEM), v_second)
        new = (w_in_new, w_out_new, m_in_new, m_out_new, v_in_new, v_out_new)
        return *(array[None] for array in new), y_next[None]

    in_specs = (weight_spec,) * 6 + (acc_spec, acc_spec, P("stage", "data", None), P("data", None), P(None, "data", None), P())
    out_specs = (weight_spec,) * 6 + (P(None, "data", None),)
    return jax.shard_map(local_step, mesh=mesh, in_specs=in_specs, out_specs=out_specs, check_vma=False)
```

```python
import math

import jax
import jax.numpy as jnp
from jax import lax
from jax.experimental import pallas as pl
from jax.experimental.pallas import tpu as pltpu
from jax.sharding import PartitionSpec as P

BETA_ONE = 0.9
BETA_TWO = 0.95
ADAM_EPS = 1e-8
WEIGHT_DECAY = 0.1
LR_GAIN = 0.2
CLIP_EPS = 1e-6
STEP_COUNT = 20
MESH = pl.DeviceIdType.MESH
F32, BF16 = jnp.float32, jnp.bfloat16

D, FF, STAGES, REPLICAS, TOK = 768, 3072, 8, 4, 64
ROWS = REPLICAS * TOK
CHUNKS = 48
R1, R2 = D // CHUNKS, FF // CHUNKS
GROUP = 8
LAG = 16
TILE = 256
SLOTS = 8
EARLY = (9, 2)
HEAD = (3, 0)
DONOR = 3
VMEM_LIMIT = 19800000
FLUSH = 4
LEARN_RATE = LR_GAIN * D ** -0.5
GELU_K = math.sqrt(2.0 / math.pi)
NT = (((1,), (1,)), ((), ()))
TN = (((0,), (0,)), ((), ()))
NN = (((1,), (0,)), ((), ()))


def mm(lhs, rhs, dims):
    return lax.dot_general(lhs, rhs, dims, preferred_element_type=F32)


def gelu_parts(z):
    zz = z * z
    tanh = jnp.tanh(GELU_K * (z + 0.044715 * (zz * z)))
    cdf = 0.5 * (1.0 + tanh)
    slope = cdf + (0.5 * z) * (1.0 - tanh * tanh) * (GELU_K * (1.0 + (3 * 0.044715) * zz))
    return z * cdf, slope


def gelu(z):
    return z * (0.5 * (1.0 + jnp.tanh(GELU_K * (z + 0.044715 * (z * z * z)))))


def clip_of(sq_norm, max_norm):
    return jnp.minimum(1.0, max_norm / (jnp.sqrt(sq_norm) + CLIP_EPS))


def moments(moment, sq_moment, gradient):
    return BETA_ONE * moment + (1.0 - BETA_ONE) * gradient, BETA_TWO * sq_moment + (1.0 - BETA_TWO) * gradient * gradient


def new_weight(weight, moment_new, sq_new):
    step = (LEARN_RATE / (1.0 - BETA_ONE ** STEP_COUNT)) * moment_new
    v_hat = sq_new * (1.0 / (1.0 - BETA_TWO ** STEP_COUNT))
    return weight * (1.0 - LEARN_RATE * WEIGHT_DECAY) - step / (jnp.sqrt(v_hat) + ADAM_EPS)


def owner_of(stage):
    return 3 * ((stage % 2 + (stage // 2) % 2) % 2)


def ds(index, size):
    return pl.ds(pl.multiple_of(index * size, size), size)


def step_kernel(w1, w2, m1, m2, v1, v2, acc1, acc2, a_in, gy_in, x_in, maxn,
                recv2, own2, first_o, v2_o, g1_o, g2_o, y_o,
                b1, b2, hid, ring1, ring2, ringv, abuf, gbuf, gnext, xbuf, ybuf, sq1, sq2, nbuf, nplane,
                a_snd, a_rcv, in_snd, in_rcv, g_snd, g_rcv, x_snd, x_rcv, y_snd, y_rcv, rs_snd, ag_snd, line_rcv,
                n_snd, n_rcv, np_snd, np_rcv, nt_snd, nt_rcv, ld, st, vo, loc):
    r = lax.axis_index("data")
    s = lax.axis_index("stage")
    own_r = owner_of(s)
    away = 1 - 2 * (own_r // 3)
    d = (r - own_r) * away
    partner = s + 1 - 2 * (s % 2)
    pair, plane = s // 2, r // 3
    early = EARLY[0] + (EARLY[1] - EARLY[0]) * (s % 2)
    head = jnp.where(d == 1, HEAD[0] + (HEAD[1] - HEAD[0]) * (s % 2), 0)
    recv1, own1, sq_o = (first_o.at[i] for i in range(3))
    accs, recvs, owns, gouts = (acc1, acc2), (recv1, recv2), (own1, own2), (g1_o, g2_o)
    rings, weights_hbm, moments_hbm = (ring1, ring2), (w1, w2), (m1, m2)
    heights = (R1, R2)
    gp, dz = first_o.at[2, pl.ds(0, ROWS), :], first_o.at[2, pl.ds(ROWS, ROWS), :]

    def remote(src, dst, snd, rcv, to_r, to_s):
        return pltpu.make_async_remote_copy(src_ref=src, dst_ref=dst, send_sem=snd, recv_sem=rcv,
                                            device_id=(to_r, to_s), device_id_type=MESH)

    def arrive(ref, sem):
        pltpu.make_async_copy(ref, ref, sem).wait()

    def gather(src, dst, snd, rcv):
        part = dst.at[ds(r, TOK), :]

        @pl.when(d == 0)
        def _():
            pltpu.make_async_copy(src, part, rcv.at[r]).start()

        @pl.when(d != 0)
        def _():
            remote(src, part, snd, rcv.at[r], own_r, s).start()

    def gathered(dst, rcv):
        for q in range(REPLICAS):
            arrive(dst.at[pl.ds(q * TOK, TOK), :], rcv.at[q])

    barrier = pltpu.get_barrier_semaphore()
    for q in range(1, REPLICAS):
        pl.semaphore_signal(barrier, inc=1, device_id=((r + q) % REPLICAS, s), device_id_type=MESH)

    @pl.when(d == 0)
    def _():
        for t in range(1, STAGES):
            peer = (s + t) % STAGES
            pl.semaphore_signal(barrier, inc=1, device_id=(owner_of(peer), peer), device_id_type=MESH)

    @pl.when(s != STAGES - 1)
    def _():
        pl.semaphore_signal(barrier, inc=1, device_id=(r, STAGES - 1), device_id_type=MESH)

    @pl.when((s == STAGES - 1) & (d == 0))
    def _():
        for q in range(1, REPLICAS):
            pl.semaphore_signal(barrier, inc=1, device_id=(q, DONOR), device_id_type=MESH)

    at_end = (r == 0) | (r == REPLICAS - 1)

    @pl.when(at_end)
    def _():
        pl.semaphore_signal(barrier, inc=1, device_id=(r, partner), device_id_type=MESH)

    signals = REPLICAS - 1 + jnp.where(at_end, 1, 0) + jnp.where(d == 0, STAGES - 1, 0) + jnp.where(s == STAGES - 1, STAGES - 1, 0) + jnp.where((s == DONOR) & (d != 0), 1, 0)
    pl.semaphore_wait(barrier, signals)

    @pl.when(s == STAGES - 1)
    def _():
        @pl.when(d == 0)
        def _():
            pltpu.make_async_copy(gy_in, gbuf.at[ds(r, TOK), :], in_rcv.at[r]).start()

    @pl.when((s == DONOR) & (d != 0))
    def _():
        remote(gy_in, gbuf.at[ds(r, TOK), :], in_snd, in_rcv.at[r], 0, STAGES - 1).start()

    gather(a_in, abuf, a_snd, a_rcv)

    @pl.when(s == 0)
    def _():
        gather(x_in, xbuf, in_snd, in_rcv)

    def rs_copy(mat, k, src):
        part = recvs[mat].at[ds(k, heights[mat]), :]
        sem = mat * CHUNKS + k
        return remote(src, part, rs_snd.at[mat], line_rcv.at[sem], r - away, s)

    def rs_src(mat, k):
        return owns[mat].at[ds(k, heights[mat]), :]

    def ag_copy(mat, k, from_vmem):
        rows = ds(k, heights[mat])
        src = recvs[mat] if from_vmem else gouts[mat]
        sem = mat * CHUNKS + k
        return remote(src.at[rows, :], gouts[mat].at[rows, :], ag_snd.at[sem // GROUP], line_rcv.at[sem], r + away, s)

    def sent(mat, group):
        arrive(gouts[mat].at[ds(group, GROUP * heights[mat]), :], ag_snd.at[mat * (CHUNKS // GROUP) + group])

    def ag_range(lo, hi):
        for mat in (0, 1):
            @pl.loop(jnp.clip(lo - mat * CHUNKS, 0, CHUNKS), jnp.clip(hi - mat * CHUNKS, 0, CHUNKS))
            def _(k):
                ag_copy(mat, k, True).start()

    def each(mats, fn, lo=0, hi=CHUNKS):
        for mat in mats:
            @pl.loop(lo, hi)
            def _(k):
                fn(mat, k)

    def pass_on(mat, k):
        rows = ds(k, heights[mat])
        arrive(gouts[mat].at[rows, :], line_rcv.at[mat * CHUNKS + k])

        @pl.when(d != 3)
        def _():
            ag_copy(mat, k, False).start()

    @pl.when(d == 3)
    def _():
        parts = 4
        loads = [pltpu.make_async_copy(acc1.at[0, 0, pl.ds(q * D // parts, D // parts), :], own1.at[pl.ds(q * D // parts, D // parts), :], ld.at[0, q])
                 for q in range(parts)]
        loads.append(pltpu.make_async_copy(acc2.at[0, 0], own2, ld.at[1, 0]))
        for copy in loads:
            copy.start()
        for q in range(parts):
            loads[q].wait()
            each((0,), lambda mat, k: rs_copy(mat, k, rs_src(mat, k)).start(), q * CHUNKS // parts, (q + 1) * CHUNKS // parts)
        loads[parts].wait()
        each((1,), lambda mat, k: rs_copy(mat, k, rs_src(mat, k)).start())

    @pl.when((d == 1) | (d == 2))
    def _():
        own_copies = [pltpu.make_async_copy(accs[mat].at[0, 0], owns[mat], ld.at[mat, 0]) for mat in (0, 1)]
        for copy in own_copies:
            copy.start()
        for mat in (0, 1):
            own_copies[mat].wait()

            @pl.loop(0, CHUNKS)
            def _(k):
                rows = ds(k, heights[mat])
                arrive(recvs[mat].at[rows, :], line_rcv.at[mat * CHUNKS + k])
                recvs[mat][rows, :] = recvs[mat][rows, :] + owns[mat][rows, :]
                rs_copy(mat, k, recvs[mat].at[rows, :]).start()
                if mat == 1:
                    @pl.when(k >= CHUNKS - head)
                    def _():
                        pass_on(0, k - (CHUNKS - head))

    def load(mat, k, src, ring, sem):
        slot = k % SLOTS
        return pltpu.make_async_copy(src, ring.at[slot], st.at[sem * SLOTS + slot])

    def load_rows(mat, k, hbm):
        return load(mat, k, hbm.at[ds(k, heights[mat]), :], rings[mat], mat)

    def load_v2(k, hbm):
        return load(1, k, hbm.at[ds(k, R2), :], ringv, 2)

    def store_v2(k):
        return pltpu.make_async_copy(ringv.at[k % SLOTS], v2_o.at[ds(k, R2), :], vo.at[k % SLOTS])

    def whole(mat, src, dst, sem):
        return pltpu.make_async_copy(src.at[0], dst, ld.at[mat, sem])

    @pl.when(d != 0)
    def _():
        fills = ([whole(0, w1, recv1, 0), whole(0, m1, own1, 1), whole(0, v1, sq_o, 2)], [whole(1, w2, recv2, 0), whole(1, m2, own2, 1)])

        def prefetch():
            for mat in (0, 1):
                arrive(recvs[mat], rs_snd.at[mat])
            for copy in fills[0] + fills[1]:
                copy.start()

        @pl.when(d == 3)
        def _():
            prefetch()
            arrive(nplane.at[plane], np_rcv.at[0])
            remote(nplane.at[plane], nplane.at[plane], np_snd.at[0], np_rcv.at[1], own_r, s).start()
            arrive(nplane.at[1 - plane], np_rcv.at[2])
            for q in (1, 2):
                remote(nplane, nplane, nt_snd.at[q], nt_rcv, own_r + q * away, s).start()

        each((0,), pass_on, head, LAG // 2)

        @pl.when(d != 3)
        def _():
            prefetch()

        each((0,), pass_on, LAG // 2, LAG)

        @pl.when(d != 3)
        def _():
            arrive(nplane, nt_rcv)

        clip = clip_of(nplane[0] + nplane[1], maxn[0, 0])[0:1, 0:1]
        for copy in fills[0]:
            copy.wait()

        def update_first(k):
            load_rows(0, k, g1_o).wait()
            rows = ds(k, R1)
            moment, sq_moment = moments(own1[rows, :], sq_o[rows, :], clip * ring1[k % SLOTS])
            recv1[rows, :] = new_weight(recv1[rows, :], moment, sq_moment)
            own1[rows, :] = moment
            sq_o[rows, :] = sq_moment

        def update_second(k):
            load_rows(1, k, g2_o).wait()
            load_v2(k, v2.at[0]).wait()
            rows = ds(k, R2)
            moment, sq_moment = moments(own2[rows, :], ringv[k % SLOTS], clip * ring2[k % SLOTS])
            recv2[rows, :] = new_weight(recv2[rows, :], moment, sq_moment)
            own2[rows, :] = moment
            ringv[k % SLOTS] = sq_moment
            store_v2(k).start()

        @pl.loop(LAG, 2 * LAG)
        def _(k):
            pass_on(0, k)
            for i in (0, 1):
                load_rows(0, 2 * (k - LAG) + i, g1_o).start()

            @pl.when(k > LAG)
            def _():
                for i in (0, 1):
                    update_first(2 * (k - LAG - 1) + i)

        update_first(2 * LAG - 2)

        @pl.loop(2 * LAG, CHUNKS)
        def _(k):
            pass_on(0, k)
            load_rows(0, k, g1_o).start()
            update_first(k - 1)

        update_first(CHUNKS - 1)
        for copy in fills[1]:
            copy.wait()

        @pl.loop(0, CHUNKS)
        def _(k):
            pass_on(1, k)

            @pl.when(k >= SLOTS)
            def _():
                store_v2(k - SLOTS).wait()

            load_rows(1, k, g2_o).start()
            load_v2(k, v2.at[0]).start()

            @pl.when(k > 0)
            def _():
                update_second(k - 1)

            @pl.when((s == STAGES - 1) & (k == CHUNKS - 8))
            def _():
                arrive(y_o, y_rcv)
                for t in range(1, STAGES):
                    remote(y_o, y_o, y_snd.at[t], y_rcv, r, (s + t) % STAGES).start()

        update_second(CHUNKS - 1)
        each((1,), lambda mat, k: store_v2(k).wait(), CHUNKS - SLOTS, CHUNKS)

        @pl.when(d == 3)
        def _():
            remote(nplane.at[plane], nplane.at[plane], np_snd.at[0], np_rcv.at[1], own_r, s).wait_send()
            for q in (1, 2):
                remote(nplane, nplane, nt_snd.at[q], nt_rcv, own_r + q * away, s).wait_send()

        remote(a_in, abuf.at[ds(r, TOK), :], a_snd, a_rcv.at[r], own_r, s).wait_send()

        @pl.when((s == 0) | (s == DONOR))
        def _():
            remote(x_in, xbuf.at[ds(r, TOK), :], in_snd, in_rcv.at[r], own_r, s).wait_send()

        @pl.when(d != 3)
        def _():
            each((0, 1), sent, 0, CHUNKS // GROUP)

    @pl.when(d == 0)
    def _():
        loads = [pltpu.make_async_copy(w.at[0], own, ld.at[mat, 0]) for mat, (w, own) in enumerate(((w1, own1), (w2, own2)))]
        for copy in loads:
            copy.start()
        sq1[...] = jnp.zeros_like(sq1)
        sq2[...] = jnp.zeros_like(sq2)
        loads[0].wait()

        @pl.loop(0, CHUNKS)
        def _(k):
            b1[ds(k, R1), :] = own1[ds(k, R1), :].astype(BF16)

        loads[1].wait()

        @pl.loop(0, CHUNKS)
        def _(k):
            b2[ds(k, R2), :] = own2[ds(k, R2), :].astype(BF16)

        own_copies = [pltpu.make_async_copy(accs[mat].at[0, 0], owns[mat], ld.at[mat, 1]) for mat in (0, 1)]
        for copy in own_copies:
            copy.start()

        gathered(abuf, a_rcv)

        @pl.loop(0, FF // TILE)
        def _(j):
            cols = ds(j, TILE)
            value, slope = gelu_parts(mm(abuf[...], b1[:, cols], NN))
            hid[:, cols] = value.astype(BF16)
            gp[:, cols] = slope

        @pl.when(s == STAGES - 1)
        def _():
            gathered(gbuf, in_rcv)

        @pl.when(s != STAGES - 1)
        def _():
            arrive(gbuf, g_rcv)

        @pl.loop(0, FF // TILE)
        def _(j):
            cols = ds(j, TILE)
            dz[:, cols] = (gp[:, cols] * mm(gbuf[...], b2[cols, :], NT)).astype(BF16).astype(F32)

        send_g = remote(gnext, gbuf, g_snd, g_rcv, owner_of(s + STAGES - 1), (s + STAGES - 1) % STAGES)

        @pl.when(s != 0)
        def _():
            @pl.loop(0, D // TILE)
            def _(j):
                gnext[:, ds(j, TILE)] = mm(dz[...].astype(BF16), b1[ds(j, TILE), :], NT).astype(BF16)

            send_g.start()

        own_copies[0].wait()

        @pl.loop(0, FF // TILE)
        def _(j):
            cols = ds(j, TILE)
            own1[:, cols] = own1[:, cols] + mm(abuf[...], dz[:, cols].astype(BF16), TN)

        own_copies[1].wait()

        @pl.loop(0, FF // TILE)
        def _(j):
            cols = ds(j, TILE)
            own2[cols, :] = own2[cols, :] + mm(hid[:, cols], gbuf[...], TN)

        for mat in (0, 1):
            sq = (sq1, sq2)[mat]

            @pl.loop(0, CHUNKS)
            def _(k):
                rows = ds(k, heights[mat])
                arrive(recvs[mat].at[rows, :], line_rcv.at[mat * CHUNKS + k])
                avg = (recvs[mat][rows, :] + owns[mat][rows, :]) * (1.0 / REPLICAS)
                recvs[mat][rows, :] = avg
                part = avg[0:8, :] * avg[0:8, :]
                for i in range(1, heights[mat] // 8):
                    part = part + avg[8 * i:8 * i + 8, :] * avg[8 * i:8 * i + 8, :]
                sq[...] = sq[...] + part
                if mat == 1:
                    @pl.when(k >= CHUNKS - early)
                    def _():
                        ag_copy(0, k - (CHUNKS - early), True).start()

        chained = (s % 2 == 0) | (s == STAGES - 1)
        first = jnp.where(chained, 26 + 6 * s + s // 4 - 2 * (s // 7), 2 * CHUNKS)
        second = jnp.where(chained, first + 3, 2 * CHUNKS)
        ag_range(early, first)

        fills = [whole(0, m1, own1, 2), whole(0, v1, sq_o, 3), whole(1, m2, own2, 2)]
        for copy in fills:
            copy.start()
        for k in range(SLOTS):
            load_rows(0, k, w1.at[0]).start()
            load_rows(1, k, w2.at[0]).start()
            load_v2(k, v2.at[0]).start()

        partial = jnp.sum(sq1[...], keepdims=True) + jnp.sum(sq2[...], keepdims=True)
        nbuf[pair] = jnp.broadcast_to(partial, (8, 128))
        norm_copies = []
        for q in range(1, REPLICAS):
            other = (pair + q) % REPLICAS
            norm_copies.append(remote(nbuf.at[pair], nbuf.at[pair], n_snd.at[q], n_rcv.at[pair], r, 2 * other + (other + plane) % 2))
            norm_copies[-1].start()
        for q in range(1, REPLICAS):
            other = (pair + q) % REPLICAS
            arrive(nbuf.at[other], n_rcv.at[other])
        nplane[plane] = (nbuf[0] + nbuf[1]) + (nbuf[2] + nbuf[3])
        norm_copies.append(remote(nplane.at[plane], nplane.at[plane], np_snd.at[0], np_rcv.at[0], r, partner))
        norm_copies[-1].start()
        arrive(nplane.at[1 - plane], np_rcv.at[1])
        norm_copies.append(remote(nplane.at[1 - plane], nplane.at[1 - plane], np_snd.at[1], np_rcv.at[2], r, partner))
        norm_copies[-1].start()
        total = nplane[0] + nplane[1]

        clip = clip_of(total, maxn[0, 0])[0:1, 0:1]
        for copy in fills:
            copy.wait()

        @pl.loop(0, CHUNKS)
        def _(k):
            load_rows(0, k, w1.at[0]).wait()
            rows = ds(k, R1)
            moment, sq_moment = moments(own1[rows, :], sq_o[rows, :], clip * recv1[rows, :])
            b1[rows, :] = new_weight(ring1[k % SLOTS], moment, sq_moment).astype(BF16)
            own1[rows, :] = moment
            sq_o[rows, :] = sq_moment

            @pl.when(k + SLOTS < CHUNKS)
            def _():
                load_rows(0, k + SLOTS, w1.at[0]).start()

        @pl.loop(0, CHUNKS)
        def _(k):
            load_rows(1, k, w2.at[0]).wait()
            load_v2(k, v2.at[0]).wait()
            rows = ds(k, R2)
            moment, sq_moment = moments(own2[rows, :], ringv[k % SLOTS], clip * recv2[rows, :])
            b2[rows, :] = new_weight(ring2[k % SLOTS], moment, sq_moment).astype(BF16)
            own2[rows, :] = moment
            ringv[k % SLOTS] = sq_moment
            store_v2(k).start()

            @pl.when(k + SLOTS < CHUNKS)
            def _():
                load_rows(1, k + SLOTS, w2.at[0]).start()

            @pl.when((k >= SLOTS // 2) & (k + SLOTS // 2 < CHUNKS))
            def _():
                store_v2(k - SLOTS // 2).wait()
                load_v2(k + SLOTS // 2, v2.at[0]).start()

        each((1,), lambda mat, k: store_v2(k).wait(), CHUNKS - SLOTS, CHUNKS)

        @pl.when(s == 0)
        def _():
            gathered(xbuf, in_rcv)

        @pl.when(s != 0)
        def _():
            arrive(xbuf, x_rcv)

        ag_range(first, second)

        @pl.loop(0, FF // TILE)
        def _(j):
            cols = ds(j, TILE)
            hid[:, cols] = gelu(mm(xbuf[...], b1[:, cols], NN)).astype(BF16)

        @pl.loop(0, D // TILE)
        def _(j):
            ybuf[:, ds(j, TILE)] = mm(hid[...], b2[:, ds(j, TILE)], NN).astype(BF16)

        send_x = remote(ybuf, xbuf, x_snd, x_rcv, owner_of(s + 1), (s + 1) % STAGES)

        @pl.when(s != STAGES - 1)
        def _():
            send_x.start()

        y_rows = ybuf.at[ds(r, TOK), :]

        @pl.when(s == STAGES - 1)
        def _():
            keep = pltpu.make_async_copy(y_rows, y_o, loc.at[2])
            keep.start()
            for q in range(1, REPLICAS):
                remote(ybuf.at[ds(own_r + q * away, TOK), :], y_o, y_snd.at[q + STAGES], y_rcv, own_r + q * away, s).start()
            keep.wait()
            for t in range(1, STAGES):
                remote(y_o, y_o, y_snd.at[t], y_rcv, r, (s + t) % STAGES).start()

        ag_range(second, 2 * CHUNKS)

        @pl.when(s == STAGES - 1)
        def _():
            for q in range(1, REPLICAS):
                remote(ybuf.at[ds(own_r + q * away, TOK), :], y_o, y_snd.at[q + STAGES], y_rcv, own_r + q * away, s).wait_send()

        @pl.when(s != 0)
        def _():
            send_g.wait_send()

        @pl.when(s != STAGES - 1)
        def _():
            send_x.wait_send()

        for copy in norm_copies:
            copy.wait_send()

        for k in range(SLOTS):
            load_rows(0, k, w1.at[0]).start()
            load_rows(1, k, w2.at[0]).start()
            load_v2(k, v2_o).start()

        @pl.loop(0, CHUNKS)
        def _(k):
            @pl.when(k % GROUP == 0)
            def _():
                sent(0, k // GROUP)

            load_rows(0, k, w1.at[0]).wait()
            rows = ds(k, R1)
            recv1[rows, :] = new_weight(ring1[k % SLOTS], own1[rows, :], sq_o[rows, :])

            @pl.when(k + SLOTS < CHUNKS)
            def _():
                load_rows(0, k + SLOTS, w1.at[0]).start()

        @pl.loop(0, CHUNKS)
        def _(k):
            @pl.when(k % GROUP == 0)
            def _():
                sent(1, k // GROUP)

            load_rows(1, k, w2.at[0]).wait()
            load_v2(k, v2_o).wait()
            rows = ds(k, R2)
            recv2[rows, :] = new_weight(ring2[k % SLOTS], own2[rows, :], ringv[k % SLOTS])

            @pl.when(k + SLOTS < CHUNKS)
            def _():
                load_rows(1, k + SLOTS, w2.at[0]).start()
                load_v2(k + SLOTS, v2_o).start()

    @pl.when(s != STAGES - 1)
    def _():
        arrive(y_o, y_rcv)

    @pl.when(s == STAGES - 1)
    def _():
        for t in range(1, STAGES):
            remote(y_o, y_o, y_snd.at[t], y_rcv, r, (s + t) % STAGES).wait_send()


def flush_kernel(w_second, m_second, first, v_second, w_out, m_out, w_first, m_first, v_first, v_out, buf, rsem, wsem):
    height = FF // FLUSH

    def parts(k):
        rows = pl.ds(k * height, height)
        return (pltpu.make_async_copy(v_second.at[rows, :], buf.at[rows, :], rsem.at[k]),
                pltpu.make_async_copy(buf.at[rows, :], v_out.at[rows, :], wsem.at[k]))

    copies = [pltpu.make_async_copy(first.at[i], target, wsem.at[FLUSH + i]) for i, target in enumerate((w_first, m_first, v_first))]
    for k in range(FLUSH):
        parts(k)[0].start()
    for copy in copies:
        copy.start()
    for k in range(FLUSH):
        parts(k)[0].wait()
        parts(k)[1].start()
    for k in range(FLUSH):
        parts(k)[1].wait()
    for copy in copies:
        copy.wait()


def solution(mesh):
    assert mesh.shape["stage"] == STAGES and mesh.shape["data"] == REPLICAS
    weight_spec = P("stage", None, None)
    acc_spec = P("data", "stage", None, None)

    def local_step(w_in, w_out, mom_in, mom_out, sq_in, sq_out, acc_in, acc_out, stage_acts, grad_y, x_next, max_norm):
        maxn = max_norm.reshape(1, 1)
        hbm = pl.BlockSpec(memory_space=pl.ANY)
        vmem = pl.BlockSpec(memory_space=pltpu.VMEM)
        dma = pltpu.SemaphoreType.DMA
        tall = pltpu.VMEM((FF, D), F32)
        w_second, m_second, first, v_second, _, _, y_next = pl.pallas_call(
            step_kernel,
            out_shape=(
                tall, tall, pltpu.VMEM((3, D, FF), F32),
                jax.ShapeDtypeStruct((FF, D), F32), jax.ShapeDtypeStruct((D, FF), F32), jax.ShapeDtypeStruct((FF, D), F32),
                jax.ShapeDtypeStruct((TOK, D), BF16),
            ),
            in_specs=[hbm] * 11 + [pl.BlockSpec(memory_space=pltpu.SMEM)],
            out_specs=(vmem,) * 3 + (hbm,) * 4,
            scratch_shapes=[
                pltpu.VMEM((D, FF), BF16), pltpu.VMEM((FF, D), BF16), pltpu.VMEM((ROWS, FF), BF16),
                pltpu.VMEM((SLOTS, R1, FF), F32), pltpu.VMEM((SLOTS, R2, D), F32), pltpu.VMEM((SLOTS, R2, D), F32),
                pltpu.VMEM((ROWS, D), BF16), pltpu.VMEM((ROWS, D), BF16), pltpu.VMEM((ROWS, D), BF16),
                pltpu.VMEM((ROWS, D), BF16), pltpu.VMEM((ROWS, D), BF16),
                pltpu.VMEM((8, FF), F32), pltpu.VMEM((8, D), F32),
                pltpu.VMEM((REPLICAS, 8, 128), F32), pltpu.VMEM((2, 8, 128), F32),
                dma, dma((REPLICAS,)), dma, dma((REPLICAS,)), dma, dma, dma, dma, dma((STAGES + REPLICAS,)), dma,
                dma((2,)), dma((2 * CHUNKS // GROUP,)), dma((2 * CHUNKS,)),
                dma((REPLICAS,)), dma((REPLICAS,)), dma((2,)), dma((3,)), dma((REPLICAS,)), dma,
                dma((2, 4)), dma((3 * SLOTS,)), dma((SLOTS,)), dma((3,)),
            ],
            compiler_params=pltpu.CompilerParams(has_side_effects=True, collective_id=0, vmem_limit_bytes=VMEM_LIMIT),
            name="step",
        )(w_in, w_out, mom_in, mom_out, sq_in, sq_out, acc_in, acc_out, stage_acts[0], grad_y, x_next[0], maxn)
        wide, tall = jax.ShapeDtypeStruct((D, FF), F32), jax.ShapeDtypeStruct((FF, D), F32)
        w_out_new, m_out_new, w_in_new, m_in_new, v_in_new, v_out_new = pl.pallas_call(
            flush_kernel,
            out_shape=(tall, tall, wide, wide, wide, tall),
            in_specs=[hbm, hbm, vmem, hbm],
            out_specs=(hbm,) * 6,
            input_output_aliases={0: 0, 1: 1},
            scratch_shapes=[pltpu.VMEM((FF, D), F32), dma((FLUSH,)), dma((FLUSH + 3,))],
            compiler_params=pltpu.CompilerParams(vmem_limit_bytes=10000000),
            name="flush",
        )(w_second, m_second, pltpu.with_memory_space_constraint(first, pltpu.VMEM), v_second)
        new = (w_in_new, w_out_new, m_in_new, m_out_new, v_in_new, v_out_new)
        return *(array[None] for array in new), y_next[None]

    in_specs = (weight_spec,) * 6 + (acc_spec, acc_spec, P("stage", "data", None), P("data", None), P(None, "data", None), P())
    out_specs = (weight_spec,) * 6 + (P(None, "data", None),)
    return jax.shard_map(local_step, mesh=mesh, in_specs=in_specs, out_specs=out_specs, check_vma=False)
```
